256 devices in a mesh: col: 64 (over y, z, core), lev: 4 (over x).
Axes of the slice: x: 4, y: 4, z: 8, core: 2. Of those that a mesh axis runs over, the one named last changes fastest.
Arguments:
- state_anom: bfloat16 [48, 64, 65536], P('lev', None, 'col'), may hold values from -6 to 6
- error_sum: float32 [48, 65536], P('lev', 'col'), may hold values from -3 to 3
- obs_anom: bfloat16 [64, 131072], P('lev', 'col'), may hold values from -6 to 6
- local_weight: float32 [32, 131072], P(None, 'col'), may hold values from 0.05 to 1
- neighbours: int32 [32, 131072], P(None, 'col'), may hold values from 0 to 3071, as said below
- innovation: float32 [131072], P(('col', 'lev')), may hold values from -6 to 6
- obs_type: int32 [131072], P(('col', 'lev')), may hold values from 0 to 31
- live: int32 [131072], P(('col', 'lev')), may hold values 0 or 1
Outputs:
- impact: float32 [131072], P(('col', 'lev'))
- type_impact: float32 [32], replicated
The draws below stay inside these ranges and needn't reach their ends.
Inputs may be any that keep to these rules, and one draw needn't show every extreme that they name: Observation o lies in column tile o // 2048; the column (o // 2048 - 1) * 1024 + neighbours[n, o] lies in that tile or the tile on either side of it, inside the grid.
All inputs are finite; a program needn't handle non-finite values. No bound on the sum of `live` on one device may be relied on, other than what follows from the above.
Results may differ from the reference program's by a relative error of at most 0.0003.
Values may be sent and summed in bfloat16 or wider, within the bound.
No kernel may reach another device: no remote copies, remote signals or barrier semaphores. Data moves between devices by JAX's collectives and lax.ppermute only.
A program may use at most 64 MiB of HBM per device.

```python
import jax
import jax.numpy as jnp
from jax import lax

MEMBERS = 64
LEV = 48
NEIGH = 32
BLOCK = 128
NTYPE = 32
COL_DEV = 1024
BLK_DEV = 16
COLS = 65536
OBS_DEV = 2048
OBS = 131072
N_COL = 64


def draw_neighbours(key, part):
    slots = jnp.arange(OBS, dtype=jnp.int32)
    tile = slots // OBS_DEV
    base = (tile - 1) * COL_DEV
    lower = jnp.maximum(tile - 1, 0) * COL_DEV - base
    upper = jnp.minimum(tile + 2, N_COL) * COL_DEV - base
    lower = jnp.broadcast_to(lower[None, :], (NEIGH, OBS))
    upper = jnp.broadcast_to(upper[None, :], (NEIGH, OBS))
    return jax.random.randint(jax.random.fold_in(key, 11), (NEIGH, OBS), lower, upper, dtype=jnp.int32)


def place_ends(array, own_key, low, top_value):
    index_at = [jax.random.randint(jax.random.fold_in(own_key, axis), (), 0, length) for axis, length in enumerate(array.shape)]
    widest = array.shape.index(max(array.shape))
    next_to = index_at[:widest] + [(index_at[widest] + 1) % array.shape[widest]] + index_at[widest + 1:]
    return array.at[tuple(index_at)].set(low).at[tuple(next_to)].set(top_value)


def shard_levels(stream_key, shape, split, least, high):
    level = 1.0
    for position, blocks in split:
        draws = jax.random.uniform(jax.random.fold_in(jax.random.fold_in(stream_key, 6), position), (blocks,), jnp.float32, least / len(split), high / len(split))
        level = level * jnp.repeat(jnp.exp(draws), shape[position] // blocks).reshape((-1,) + (1,) * (len(shape) - 1 - position))
    return level


def noise(rng, dims, scale, reach, cuts=(), kind=jnp.bfloat16):
    entries = jax.random.normal(rng, dims, jnp.float32) * scale
    if len(cuts) > 0:
        entries = shard_levels(rng, dims, cuts, -0.22, 0.18) * entries
    return jnp.clip(entries, min=-reach, max=reach).astype(kind)


def setup_inputs(seed: int = 0) -> dict:
    arg_keys = jax.random.split(jax.random.key(seed), 9)
    state_anom = noise(arg_keys[0], (LEV, MEMBERS, COLS), 1.0, 6.0, ((0, 4), (2, 64)))
    error_sum = noise(arg_keys[1], (LEV, COLS), 0.2, 3.0, ((0, 4), (1, 64)), jnp.float32)
    obs_anom = noise(arg_keys[2], (MEMBERS, OBS), 1.0, 6.0, ((0, 4), (1, 64)))
    local_weight = jnp.clip(0.05 + 0.95 * jax.random.uniform(arg_keys[3], (NEIGH, OBS), jnp.float32) ** shard_levels(arg_keys[3], (NEIGH, OBS), ((1, 64),), -0.2, 0.2), 0.05, 1.0)
    neighbours = draw_neighbours(jax.random.fold_in(arg_keys[8], 71), 0)
    innovation = noise(arg_keys[5], (OBS,), 1.0, 6.0, ((0, 256),), jnp.float32)
    obs_type = place_ends(jax.random.randint(arg_keys[6], (OBS,), 0, NTYPE), jax.random.fold_in(arg_keys[6], 1), 0, NTYPE - 1).astype(jnp.int32)
    live = place_ends((jax.random.randint(arg_keys[7], (OBS,), 0, 4) < 3).astype(jnp.int32), jax.random.fold_in(arg_keys[7], 1), 0, 1)
    return {"state_anom": state_anom, "error_sum": error_sum, "obs_anom": obs_anom, "local_weight": local_weight, "neighbours": neighbours, "innovation": innovation, "obs_type": obs_type, "live": live}


def reference(state_anom, error_sum, obs_anom, local_weight, neighbours, innovation, obs_type, live):
    sens = jnp.einsum("lkc,lc->kc", state_anom.astype(jnp.float32), error_sum, precision=lax.Precision.HIGHEST)
    step_rows = BLOCK * BLK_DEV
    count = OBS // step_rows
    anom_blocks = jnp.transpose(obs_anom.reshape(MEMBERS, count, step_rows), (1, 0, 2))
    weight_blocks = jnp.transpose(local_weight.reshape(NEIGH, count, step_rows), (1, 0, 2))
    index_blocks = jnp.transpose(neighbours.reshape(NEIGH, count, step_rows), (1, 0, 2))
    tile_ids = jnp.arange(count, dtype=jnp.int32)

    def one_block(items):
        anom, weight, index, tile = items
        start = ((tile - 1) * COL_DEV).astype(jnp.int32)
        picked = jnp.take(sens, (index + start).astype(jnp.int32), axis=1)
        spread = jnp.einsum("kno,no->ko", picked, weight, precision=lax.Precision.HIGHEST)
        return jnp.sum(anom.astype(jnp.float32) * spread, axis=0)

    pair = lax.map(one_block, (anom_blocks, weight_blocks, index_blocks, tile_ids)).reshape(OBS)
    impact = pair * innovation * live.astype(jnp.float32) / (MEMBERS - 1.0)
    onehot = (obs_type[None, :] == jnp.arange(NTYPE, dtype=jnp.int32)[:, None]).astype(jnp.float32)
    type_impact = jnp.sum(onehot * impact[None, :], axis=1)
    return impact, type_impact
```

```python
import jax
import jax.numpy as jnp
from jax import lax
from jax.experimental import pallas as pl
from jax.experimental.pallas import tpu as pltpu
from jax.sharding import Mesh
from jax.sharding import PartitionSpec as P

MEMBERS = 64
NTYPE = 32
COL = ("col_0", "col_1", "col_2")
COL_LEV = ("col_0", "col_1", "col_2", "lev")
GROUPS = 4
TILE = 128
F32 = jnp.float32
BF16 = jnp.bfloat16
VMEM = pl.BlockSpec(memory_space=pltpu.VMEM)


def hi_lo(x):
    hi = x.astype(BF16)
    lo = (x - hi.astype(F32)).astype(BF16)
    return jnp.concatenate([hi, lo], axis=0)


def pack_kernel(state, error, anom, out):
    total = state[0].astype(F32) * error[0:1, :]
    for level in range(1, state.shape[0]):
        total += state[level].astype(F32) * error[level : level + 1, :]
    members, width = total.shape
    out[0, 0 : 2 * members, :] = hi_lo(total)
    rows = anom.shape[0]
    for chunk in range(anom.shape[1] // width):
        at = 2 * members + chunk * rows
        out[0, at : at + rows, :] = anom[:, chunk * width : (chunk + 1) * width]


def pack(state, error, anom):
    levels, members, columns = state.shape
    width = columns // GROUPS
    rows, slots = anom.shape
    height = 2 * members + rows * slots // width
    return pl.pallas_call(
        pack_kernel,
        grid=(GROUPS,),
        in_specs=[
            pl.BlockSpec((levels, members, width), lambda q: (0, 0, q)),
            pl.BlockSpec((levels, width), lambda q: (0, q)),
            pl.BlockSpec((rows, slots), lambda q: (0, 0)),
        ],
        out_specs=pl.BlockSpec((1, height, width), lambda q: (q, 0, 0)),
        out_shape=jax.ShapeDtypeStruct((GROUPS, height, width), BF16),
        name="pack",
    )(state, error, anom)


def total_kernel(parts, out):
    half = out.shape[0] // 2
    total = parts[0, 0:half, :].astype(F32) + parts[0, half:, :].astype(F32)
    for group in range(1, GROUPS):
        total += parts[group, 0:half, :].astype(F32) + parts[group, half:, :].astype(F32)
    out[...] = hi_lo(total)


def total_sens(parts):
    width = parts.shape[2]
    return pl.pallas_call(
        total_kernel,
        grid=(1,),
        in_specs=[pl.BlockSpec((GROUPS, 2 * MEMBERS, width), lambda i: (0, 0, 0))],
        out_specs=pl.BlockSpec((2 * MEMBERS, width), lambda i: (0, 0)),
        out_shape=jax.ShapeDtypeStruct((2 * MEMBERS, width), BF16),
        name="total",
    )(parts)


def pairs_kernel(group, left, mid, right, parts, index, weight, out):
    width = mid.shape[1]
    per = width // TILE
    chunks = out.shape[1] // width
    first = group[0] * per
    neigh = index.shape[0]

    @pl.loop(0, chunks)
    def _(chunk):
        row = pl.multiple_of(2 * MEMBERS + chunk * 16, 16)
        anom = jnp.concatenate([parts[g, pl.ds(row, 16), :] for g in range(GROUPS)], axis=0)
        anom = jnp.concatenate([anom, anom], axis=0)
        spread = [
            lax.dot_general(anom, side[...], (((0,), (0,)), ((), ())), preferred_element_type=F32)
            for side in (left, mid, right)
        ]
        for t in range(per):
            at = pl.multiple_of(chunk * width + t * TILE, TILE)
            idx = index[:, pl.ds(at, TILE)]
            idx = jnp.concatenate([idx] * (TILE // neigh), axis=0).T
            lane = idx & (TILE - 1)
            block = (idx >> 7) - first
            picked = jnp.zeros((TILE, TILE), F32)
            for side in range(3):
                for h in range(per):
                    source = spread[side][t * TILE : (t + 1) * TILE, h * TILE : (h + 1) * TILE]
                    got = jnp.take_along_axis(source, lane, axis=1, mode="promise_in_bounds")
                    picked = jnp.where(block == side * GROUPS * per + h, got, picked)
            picked = picked.T[0:neigh, :]
            pair = jnp.sum(picked * weight[:, pl.ds(at, TILE)], axis=0, keepdims=True)
            out[:, pl.ds(at, TILE)] = pair


def pairs(group, left, mid, right, parts, index, weight):
    slots = index.shape[1]
    return pl.pallas_call(
        pairs_kernel,
        in_specs=[pl.BlockSpec(memory_space=pltpu.SMEM)] + [VMEM] * 6,
        out_specs=VMEM,
        out_shape=jax.ShapeDtypeStruct((1, slots), F32),
        name="pairs",
    )(group, left, mid, right, parts, index, weight)


def shards(state_anom, error_sum, obs_anom, local_weight, neighbours, innovation, obs_type, live):
    send = pack(state_anom, error_sum, obs_anom)
    parts = lax.all_to_all(send, "lev", 0, 0, tiled=True)
    mid = total_sens(parts)
    ends = lax.axis_size(COL) - 1
    left = lax.ppermute(mid, COL, [(i, i + 1) for i in range(ends)])
    right = lax.ppermute(mid, COL, [(i + 1, i) for i in range(ends)])
    group = lax.axis_index("lev").reshape(1)
    share = pairs(group, left, mid, right, parts, neighbours, local_weight)
    got = lax.all_to_all(share.reshape(GROUPS, 1, -1), "lev", 0, 0, tiled=True)
    pair = jnp.sum(got, axis=(0, 1))
    impact = pair * innovation * live.astype(F32) / (MEMBERS - 1.0)
    onehot = (obs_type[None, :] == jnp.arange(NTYPE, dtype=jnp.int32)[:, None]).astype(F32)
    type_part = jnp.sum(onehot * impact[None, :], axis=1)
    count = lax.axis_size(COL_LEV)
    spread = jnp.broadcast_to(type_part[None, None, :], (count, 1, NTYPE))
    type_impact = jnp.sum(lax.all_to_all(spread, COL_LEV, 0, 0, tiled=True), axis=(0, 1))
    return (impact, type_impact)


def solution(mesh):
    split = Mesh(
        mesh.devices.reshape(4, 8, 2, mesh.shape["lev"]), ("col_0", "col_1", "col_2", "lev")
    )
    return jax.shard_map(
        shards,
        mesh=split,
        in_specs=(
            P("lev", None, COL),
            P("lev", COL),
            P("lev", COL),
            P(None, COL),
            P(None, COL),
            P(COL_LEV),
            P(COL_LEV),
            P(COL_LEV),
        ),
        out_specs=(P(COL_LEV), P()),
        check_vma=False,
    )
```

```python
import functools

import jax
import jax.numpy as jnp
from jax import lax
from jax.experimental import pallas as pl
from jax.experimental.pallas import tpu as pltpu
from jax.sharding import Mesh
from jax.sharding import PartitionSpec as P

MEMBERS = 64
NTYPE = 32
COL = ("col_0", "col_1", "col_2")
COL_LEV = ("col_0", "col_1", "col_2", "lev")
GROUPS = 4
CORES = 2
LANES = 128
ROWS = 8
QUARTER = 256
F32 = jnp.float32
BF16 = jnp.bfloat16
VMEM = pl.BlockSpec(memory_space=pltpu.VMEM)
SMEM = pl.BlockSpec(memory_space=pltpu.SMEM)
ANY = pl.BlockSpec(memory_space=pl.ANY)


def near(x):
    return pltpu.with_memory_space_constraint(x, pltpu.VMEM)


def halves(x, axis):
    hi = x.astype(BF16)
    lo = (x - hi.astype(F32)).astype(BF16)
    return jnp.concatenate([hi, lo], axis=axis)


def pack_kernel(state, error, anom, innovation, live, kind, out, s_buf, e_buf, a_buf, m_buf, sems):
    levels = state.shape[0]
    copies = [
        pltpu.make_async_copy(error, e_buf, sems.at[0]),
        pltpu.make_async_copy(anom, a_buf, sems.at[1]),
        pltpu.make_async_copy(innovation, m_buf.at[0], sems.at[2]),
    ]
    parts = [
        pltpu.make_async_copy(
            state.at[:, :, q * QUARTER : (q + 1) * QUARTER], s_buf.at[q], sems.at[3 + q]
        )
        for q in range(GROUPS)
    ]
    copies[0].start()
    parts[0].start()
    parts[1].start()
    copies[1].start()
    copies[2].start()
    parts[2].start()
    parts[3].start()
    copies[0].wait()
    for q in range(GROUPS):
        parts[q].wait()
        cols = slice(q * QUARTER, (q + 1) * QUARTER)
        total = s_buf[q, 0].astype(F32) * e_buf[0:1, cols]
        for level in range(1, levels):
            total += s_buf[q, level].astype(F32) * e_buf[level : level + 1, cols]
        out[q, 0 : 2 * MEMBERS, :] = halves(total, 0)
    copies[1].wait()
    copies[2].wait()
    rows = anom.shape[0]
    factor = m_buf[0] * live[...].astype(F32) / (MEMBERS - 1.0)
    upper = factor.astype(BF16).astype(F32)
    meta = jnp.concatenate(
        [upper, factor - upper, kind[...].astype(F32), jnp.zeros_like(factor)], axis=0
    ).astype(BF16)
    meta = jnp.concatenate([meta, jnp.zeros_like(meta)], axis=1)
    for q in range(GROUPS):
        for chunk in range(anom.shape[1] // QUARTER):
            at = 2 * MEMBERS + chunk * rows
            out[q, at : at + rows, :] = a_buf[:, chunk * QUARTER : (chunk + 1) * QUARTER]
        out[q, 4 * MEMBERS : 4 * MEMBERS + 16, :] = meta


def pack(state, error, anom, innovation, live, kind):
    levels = state.shape[0]
    return pl.pallas_call(
        pack_kernel,
        in_specs=[ANY, ANY, ANY, ANY, VMEM, VMEM],
        out_specs=VMEM,
        out_shape=pltpu.VMEM((GROUPS, 4 * MEMBERS + 16, QUARTER), BF16),
        scratch_shapes=[
            pltpu.VMEM((GROUPS, levels, MEMBERS, QUARTER), BF16),
            pltpu.VMEM(error.shape, F32),
            pltpu.VMEM(anom.shape, BF16),
            pltpu.VMEM((1,) + innovation.shape, F32),
            pltpu.SemaphoreType.DMA((3 + GROUPS,)),
        ],
        name="pack",
    )(state, error, anom, innovation, live, kind)


def total_kernel(parts, out):
    half = MEMBERS
    total = parts[0, 0:half, :].astype(F32) + parts[0, half : 2 * half, :].astype(F32)
    for group in range(1, GROUPS):
        total += parts[group, 0:half, :].astype(F32) + parts[group, half : 2 * half, :].astype(F32)
    out[...] = halves(total.T, 1)


def total_sens(parts):
    return pl.pallas_call(
        total_kernel,
        in_specs=[VMEM],
        out_specs=VMEM,
        out_shape=pltpu.VMEM((QUARTER, 2 * MEMBERS), BF16),
        name="total",
    )(near(parts))


def choose(rows, bits):
    for bit in bits:
        rows = [jnp.where(bit, rows[i + 1], rows[i]) for i in range(0, len(rows), 2)]
    return rows[0]


def fill(chunk, tables, parts, spread):
    at = pl.multiple_of(2 * MEMBERS + chunk * 16, 16)
    anom = jnp.concatenate([parts[g, pl.ds(at, 16), :] for g in range(GROUPS)], axis=0)
    anom = jnp.concatenate([anom, anom], axis=0)
    for side, table in enumerate(tables):
        spread[side * QUARTER : (side + 1) * QUARTER, :] = jnp.dot(
            table[...], anom, preferred_element_type=F32
        )


def consume(chunk, bases, spread, index, weight, pair, first):
    for half in range(QUARTER // LANES):
        at = pl.multiple_of(chunk * QUARTER + half * LANES, LANES)
        lanes = slice(half * LANES, (half + 1) * LANES)
        acc = jnp.zeros((ROWS, LANES), F32)
        for n in range(0, index.shape[0], ROWS):
            idx = index[n : n + ROWS, pl.ds(at, LANES)]
            row = idx & (ROWS - 1)
            bits = [(idx & (ROWS << k)) != 0 for k in range(5)]
            block = idx >> 8
            value = jnp.zeros((ROWS, LANES), F32)
            for side, base in enumerate(bases):
                got = [
                    jnp.take_along_axis(
                        spread[side * QUARTER + v * ROWS : side * QUARTER + (v + 1) * ROWS, lanes],
                        row,
                        axis=0,
                        mode="promise_in_bounds",
                    )
                    for v in range(QUARTER // ROWS)
                ]
                value = jnp.where(block == base, choose(got, bits), value)
            acc += value * weight[n : n + ROWS, pl.ds(at, LANES)]
        total = jnp.sum(acc, axis=0, keepdims=True)
        line = chunk * (QUARTER // LANES) + half
        pair[pl.ds(line, 1), :] = total if first is None else first[pl.ds(line, 1), :] + total


def pick(bases, tables, parts, index, weight, pair, first, even, odd):
    chunks = index.shape[1] // QUARTER
    fill(0, tables, parts, even)

    @pl.loop(0, chunks // 2)
    def _(step):
        fill(2 * step + 1, tables, parts, odd)
        consume(2 * step, bases, even, index, weight, pair, first)
        fill(jnp.minimum(2 * step + 2, chunks - 1), tables, parts, even)
        consume(2 * step + 1, bases, odd, index, weight, pair, first)


def near_kernel(lev, core, mid, mate, parts, index, weight, out, even, odd):
    group = lev[0]
    side = jnp.where(core[0] == 0, 2, 0)
    bases = (GROUPS + group, side * GROUPS + group)
    pick(bases, (mid, mate), parts, index, weight, out, None, even, odd)


def far_kernel(lev, core, far, parts, index, weight, first, out, even, odd, pair):
    group = lev[0]
    side = jnp.where(core[0] == 0, 0, 2)
    pick((side * GROUPS + group,), (far,), parts, index, weight, pair, first, even, odd)
    kinds = lax.broadcasted_iota(jnp.int32, (NTYPE, LANES), 0).astype(F32)
    sums = jnp.zeros((NTYPE, LANES), F32)
    per = pair.shape[0] // GROUPS
    for g in range(GROUPS):
        meta = parts[g, 4 * MEMBERS : 4 * MEMBERS + 16, 0:LANES].astype(F32)
        share = pair[g * per : (g + 1) * per, :] * (meta[0:per] + meta[per : 2 * per])
        for r in range(per):
            same = meta[2 * per + r : 2 * per + r + 1] == kinds
            sums += jnp.where(same, share[r : r + 1], 0.0)
    sums = jnp.sum(sums.T, axis=0, keepdims=True)
    tail = jnp.concatenate([sums, jnp.zeros((1, LANES - NTYPE), F32)], axis=1)
    tail = jnp.concatenate([tail, jnp.zeros((ROWS - per - 1, LANES), F32)], axis=0)
    for c in range(CORES):
        for g in range(GROUPS):
            mine = pair[g * per : (g + 1) * per, :]
            to = c * GROUPS + g
            out[to, 0:per, :] = jnp.where(core[0] == c, mine, 0.0)
            out[to, per:ROWS, :] = tail


def shards(state_anom, error_sum, obs_anom, local_weight, neighbours, innovation, obs_type, live):
    lines = innovation.shape[0] // LANES
    send = pack(
        state_anom,
        error_sum,
        obs_anom,
        innovation.reshape(lines, LANES),
        live.reshape(lines, LANES),
        obs_type.reshape(lines, LANES),
    )
    parts = lax.all_to_all(send, "lev", 0, 0, tiled=True)
    mid = total_sens(parts)
    pairs = lax.axis_size(COL) // CORES
    odd_even = [(CORES * i + 1, CORES * i + 2) for i in range(pairs - 1)]
    far = lax.ppermute(mid, COL, odd_even + [(b, a) for a, b in odd_even])
    mate = lax.ppermute(mid, "col_2", [(0, 1), (1, 0)])
    lev = lax.axis_index("lev").reshape(1)
    core = lax.axis_index("col_2").reshape(1)
    slots = neighbours.shape[1]
    index, weight, parts = near(neighbours), near(local_weight), near(parts)
    cost = functools.partial(pl.CostEstimate, bytes_accessed=1 << 20, transcendentals=0)
    first = pl.pallas_call(
        near_kernel,
        in_specs=[SMEM, SMEM] + [VMEM] * 5,
        out_specs=VMEM,
        out_shape=pltpu.VMEM((slots // LANES, LANES), F32),
        scratch_shapes=[pltpu.VMEM((2 * QUARTER, QUARTER), F32)] * 2,
        cost_estimate=cost(flops=1 << 27),
        name="near",
    )(lev, core, near(mid), near(mate), parts, index, weight)
    share = pl.pallas_call(
        far_kernel,
        in_specs=[SMEM, SMEM] + [VMEM] * 5,
        out_specs=VMEM,
        out_shape=pltpu.VMEM((CORES * GROUPS, ROWS, LANES), F32),
        scratch_shapes=[pltpu.VMEM((QUARTER, QUARTER), F32)] * 2
        + [pltpu.VMEM((slots // LANES, LANES), F32)],
        cost_estimate=cost(flops=1 << 26),
        name="far",
    )(lev, core, near(far), parts, index, weight, near(first))
    got = jnp.sum(lax.all_to_all(share, ("col_2", "lev"), 0, 0, tiled=True), axis=0)
    pair = got[0:lines].reshape(-1)
    impact = pair * innovation * live.astype(F32) / (MEMBERS - 1.0)
    chips = ("col_0", "col_1")
    spread = jnp.broadcast_to(got[lines : lines + 1][None], (lax.axis_size(chips), 1, LANES))
    type_impact = jnp.sum(lax.all_to_all(spread, chips, 0, 0, tiled=True), axis=(0, 1))[0:NTYPE]
    return (impact, type_impact)


def solution(mesh):
    split = Mesh(
        mesh.devices.reshape(4, 8, 2, mesh.shape["lev"]), ("col_0", "col_1", "col_2", "lev")
    )
    return jax.shard_map(
        shards,
        mesh=split,
        in_specs=(
            P("lev", None, COL),
            P("lev", COL),
            P("lev", COL),
            P(None, COL),
            P(None, COL),
            P(COL_LEV),
            P(COL_LEV),
            P(COL_LEV),
        ),
        out_specs=(P(COL_LEV), P()),
        check_vma=False,
    )
```

```python
import functools

import jax
import jax.numpy as jnp
from jax import lax
from jax.experimental import pallas as pl
from jax.experimental.pallas import tpu as pltpu
from jax.sharding import Mesh
from jax.sharding import PartitionSpec as P

MEMBERS = 64
NTYPE = 32
COL = ("col_0", "col_1", "col_2")
COL_LEV = ("col_0", "col_1", "col_2", "lev")
GROUPS = 4
CORES = 2
LANES = 128
ROWS = 8
QUARTER = 256
F32 = jnp.float32
BF16 = jnp.bfloat16
VMEM = pl.BlockSpec(memory_space=pltpu.VMEM)
SMEM = pl.BlockSpec(memory_space=pltpu.SMEM)
ANY = pl.BlockSpec(memory_space=pl.ANY)


def near(x):
    return pltpu.with_memory_space_constraint(x, pltpu.VMEM)


def halves(x, axis):
    hi = x.astype(BF16)
    lo = (x - hi.astype(F32)).astype(BF16)
    return jnp.concatenate([hi, lo], axis=axis)


def pack_kernel(state, error, anom, innovation, live, kind, out, s_buf, e_buf, a_buf, m_buf, sems):
    levels = state.shape[0]
    copies = [
        pltpu.make_async_copy(error, e_buf, sems.at[0]),
        pltpu.make_async_copy(anom, a_buf, sems.at[1]),
        pltpu.make_async_copy(innovation, m_buf.at[0], sems.at[2]),
    ]
    parts = [
        pltpu.make_async_copy(
            state.at[:, :, q * QUARTER : (q + 1) * QUARTER], s_buf.at[q], sems.at[3 + q]
        )
        for q in range(GROUPS)
    ]
    copies[0].start()
    parts[0].start()
    parts[1].start()
    copies[1].start()
    copies[2].start()
    parts[2].start()
    parts[3].start()
    copies[0].wait()
    for q in range(GROUPS):
        parts[q].wait()
        cols = slice(q * QUARTER, (q + 1) * QUARTER)
        total = s_buf[q, 0].astype(F32) * e_buf[0:1, cols]
        for level in range(1, levels):
            total += s_buf[q, level].astype(F32) * e_buf[level : level + 1, cols]
        out[q, 0 : 2 * MEMBERS, :] = halves(total, 0)
    copies[1].wait()
    copies[2].wait()
    rows = anom.shape[0]
    factor = m_buf[0] * live[...].astype(F32) / (MEMBERS - 1.0)
    upper = factor.astype(BF16).astype(F32)
    meta = jnp.concatenate(
        [upper, factor - upper, kind[...].astype(F32), jnp.zeros_like(factor)], axis=0
    ).astype(BF16)
    meta = jnp.concatenate([meta, jnp.zeros_like(meta)], axis=1)
    for q in range(GROUPS):
        for chunk in range(anom.shape[1] // QUARTER):
            at = 2 * MEMBERS + chunk * rows
            out[q, at : at + rows, :] = a_buf[:, chunk * QUARTER : (chunk + 1) * QUARTER]
        out[q, 4 * MEMBERS : 4 * MEMBERS + 16, :] = meta


def pack(state, error, anom, innovation, live, kind):
    levels = state.shape[0]
    return pl.pallas_call(
        pack_kernel,
        in_specs=[ANY, ANY, ANY, ANY, VMEM, VMEM],
        out_specs=VMEM,
        out_shape=pltpu.VMEM((GROUPS, 4 * MEMBERS + 16, QUARTER), BF16),
        scratch_shapes=[
            pltpu.VMEM((GROUPS, levels, MEMBERS, QUARTER), BF16),
            pltpu.VMEM(error.shape, F32),
            pltpu.VMEM(anom.shape, BF16),
            pltpu.VMEM((1,) + innovation.shape, F32),
            pltpu.SemaphoreType.DMA((3 + GROUPS,)),
        ],
        name="pack",
    )(state, error, anom, innovation, live, kind)


def total_kernel(parts, out):
    half = MEMBERS
    total = parts[0, 0:half, :].astype(F32) + parts[0, half : 2 * half, :].astype(F32)
    for group in range(1, GROUPS):
        total += parts[group, 0:half, :].astype(F32) + parts[group, half : 2 * half, :].astype(F32)
    out[...] = halves(total.T, 1)


def total_sens(parts):
    return pl.pallas_call(
        total_kernel,
        in_specs=[VMEM],
        out_specs=VMEM,
        out_shape=pltpu.VMEM((QUARTER, 2 * MEMBERS), BF16),
        name="total",
    )(near(parts))


def choose(rows, bits):
    for bit in bits:
        rows = [jnp.where(bit, rows[i + 1], rows[i]) for i in range(0, len(rows), 2)]
    return rows[0]


def fill(chunk, tables, parts, spread):
    at = pl.multiple_of(2 * MEMBERS + chunk * 16, 16)
    anom = jnp.concatenate([parts[g, pl.ds(at, 16), :] for g in range(GROUPS)], axis=0)
    anom = jnp.concatenate([anom, anom], axis=0)
    for side, table in enumerate(tables):
        spread[side * QUARTER : (side + 1) * QUARTER, :] = jnp.dot(
            table[...], anom, preferred_element_type=F32
        )


def consume(chunk, bases, spread, index, weight, pair, first):
    for half in range(QUARTER // LANES):
        at = pl.multiple_of(chunk * QUARTER + half * LANES, LANES)
        lanes = slice(half * LANES, (half + 1) * LANES)
        acc = jnp.zeros((ROWS, LANES), F32)
        for n in range(0, index.shape[0], ROWS):
            idx = index[n : n + ROWS, pl.ds(at, LANES)]
            row = idx & (ROWS - 1)
            bits = [(idx & (ROWS << k)) != 0 for k in range(5)]
            block = idx >> 8
            value = jnp.zeros((ROWS, LANES), F32)
            for side, base in enumerate(bases):
                got = [
                    jnp.take_along_axis(
                        spread[side * QUARTER + v * ROWS : side * QUARTER + (v + 1) * ROWS, lanes],
                        row,
                        axis=0,
                        mode="promise_in_bounds",
                    )
                    for v in range(QUARTER // ROWS)
                ]
                value = jnp.where(block == base, choose(got, bits), value)
            acc += value * weight[n : n + ROWS, pl.ds(at, LANES)]
        total = jnp.sum(acc, axis=0, keepdims=True)
        line = chunk * (QUARTER // LANES) + half
        pair[pl.ds(line, 1), :] = total if first is None else first[pl.ds(line, 1), :] + total


def pick(bases, tables, parts, index, weight, pair, first, even, odd):
    chunks = index.shape[1] // QUARTER
    fill(0, tables, parts, even)

    @pl.loop(0, chunks // 2)
    def _(step):
        fill(2 * step + 1, tables, parts, odd)
        consume(2 * step, bases, even, index, weight, pair, first)
        fill(jnp.minimum(2 * step + 2, chunks - 1), tables, parts, even)
        consume(2 * step + 1, bases, odd, index, weight, pair, first)


def near_kernel(lev, core, mid, mate, parts, index, weight, out, even, odd):
    group = lev[0]
    side = jnp.where(core[0] == 0, 2, 0)
    bases = (GROUPS + group, side * GROUPS + group)
    pick(bases, (mid, mate), parts, index, weight, out, None, even, odd)


def far_kernel(lev, core, far, parts, index, weight, first, out, even, odd, pair):
    group = lev[0]
    side = jnp.where(core[0] == 0, 0, 2)
    pick((side * GROUPS + group,), (far,), parts, index, weight, pair, first, even, odd)
    kinds = lax.broadcasted_iota(jnp.int32, (NTYPE, LANES), 0).astype(F32)
    sums = jnp.zeros((NTYPE, LANES), F32)
    per = pair.shape[0] // GROUPS
    for g in range(GROUPS):
        meta = parts[g, 4 * MEMBERS : 4 * MEMBERS + 16, 0:LANES].astype(F32)
        share = pair[g * per : (g + 1) * per, :] * (meta[0:per] + meta[per : 2 * per])
        for r in range(per):
            same = meta[2 * per + r : 2 * per + r + 1] == kinds
            sums += jnp.where(same, share[r : r + 1], 0.0)
    sums = jnp.sum(sums.T, axis=0, keepdims=True)
    tail = jnp.concatenate([sums, jnp.zeros((1, LANES - NTYPE), F32)], axis=1)
    tail = jnp.concatenate([tail, jnp.zeros((ROWS - per - 1, LANES), F32)], axis=0)
    for c in range(CORES):
        for g in range(GROUPS):
            mine = pair[g * per : (g + 1) * per, :]
            to = c * GROUPS + g
            out[to, 0:per, :] = jnp.where(core[0] == c, mine, 0.0)
            out[to, per:ROWS, :] = tail


def finish_kernel(got, innovation, live, impact, spread):
    lines = innovation.shape[0]
    total = got[0]
    for peer in range(1, got.shape[0]):
        total += got[peer]
    pair = total[0:lines, :]
    impact[...] = pair * innovation[...] * live[...].astype(F32) / (MEMBERS - 1.0)
    for chip in range(spread.shape[0]):
        spread[chip] = total[lines : lines + 1, :]


def last_kernel(sums, impact, impact_out, type_out):
    total = sums[0]
    for chip in range(1, sums.shape[0]):
        total += sums[chip]
    type_out[...] = total[:, 0:NTYPE]
    impact_out[...] = impact[...]


def shards(state_anom, error_sum, obs_anom, local_weight, neighbours, innovation, obs_type, live):
    lines = innovation.shape[0] // LANES
    send = pack(
        state_anom,
        error_sum,
        obs_anom,
        innovation.reshape(lines, LANES),
        live.reshape(lines, LANES),
        obs_type.reshape(lines, LANES),
    )
    parts = lax.all_to_all(send, "lev", 0, 0, tiled=True)
    mid = total_sens(parts)
    pairs = lax.axis_size(COL) // CORES
    odd_even = [(CORES * i + 1, CORES * i + 2) for i in range(pairs - 1)]
    far = lax.ppermute(mid, COL, odd_even + [(b, a) for a, b in odd_even])
    mate = lax.ppermute(mid, "col_2", [(0, 1), (1, 0)])
    lev = lax.axis_index("lev").reshape(1)
    core = lax.axis_index("col_2").reshape(1)
    slots = neighbours.shape[1]
    index, weight, parts = near(neighbours), near(local_weight), near(parts)
    cost = functools.partial(pl.CostEstimate, bytes_accessed=1 << 20, transcendentals=0)
    first = pl.pallas_call(
        near_kernel,
        in_specs=[SMEM, SMEM] + [VMEM] * 5,
        out_specs=VMEM,
        out_shape=pltpu.VMEM((slots // LANES, LANES), F32),
        scratch_shapes=[pltpu.VMEM((2 * QUARTER, QUARTER), F32)] * 2,
        cost_estimate=cost(flops=1 << 27),
        name="near",
    )(lev, core, near(mid), near(mate), parts, index, weight)
    share = pl.pallas_call(
        far_kernel,
        in_specs=[SMEM, SMEM] + [VMEM] * 5,
        out_specs=VMEM,
        out_shape=pltpu.VMEM((CORES * GROUPS, ROWS, LANES), F32),
        scratch_shapes=[pltpu.VMEM((QUARTER, QUARTER), F32)] * 2
        + [pltpu.VMEM((slots // LANES, LANES), F32)],
        cost_estimate=cost(flops=1 << 26),
        name="far",
    )(lev, core, near(far), parts, index, weight, near(first))
    got = lax.all_to_all(share, ("col_2", "lev"), 0, 0, tiled=True)
    chips = ("col_0", "col_1")
    impact, spread = pl.pallas_call(
        finish_kernel,
        in_specs=[VMEM] * 3,
        out_specs=[VMEM] * 2,
        out_shape=[
            pltpu.VMEM((lines, LANES), F32),
            pltpu.VMEM((lax.axis_size(chips), 1, LANES), F32),
        ],
        name="finish",
    )(near(got), near(innovation.reshape(lines, LANES)), near(live.reshape(lines, LANES)))
    sums = lax.all_to_all(spread, chips, 0, 0, tiled=True)
    impact, type_impact = pl.pallas_call(
        last_kernel,
        in_specs=[VMEM] * 2,
        out_specs=[VMEM] * 2,
        out_shape=[
            jax.ShapeDtypeStruct((lines, LANES), F32),
            jax.ShapeDtypeStruct((1, NTYPE), F32),
        ],
        name="last",
    )(near(sums), near(impact))
    return (impact.reshape(-1), type_impact.reshape(-1))


def solution(mesh):
    split = Mesh(
        mesh.devices.reshape(4, 8, 2, mesh.shape["lev"]), ("col_0", "col_1", "col_2", "lev")
    )
    return jax.shard_map(
        shards,
        mesh=split,
        in_specs=(
            P("lev", None, COL),
            P("lev", COL),
            P("lev", COL),
            P(None, COL),
            P(None, COL),
            P(COL_LEV),
            P(COL_LEV),
            P(COL_LEV),
        ),
        out_specs=(P(COL_LEV), P()),
        check_vma=False,
    )
```

```python
import functools

import jax
import jax.numpy as jnp
from jax import lax
from jax.experimental import pallas as pl
from jax.experimental.pallas import tpu as pltpu
from jax.sharding import Mesh
from jax.sharding import PartitionSpec as P

MEMBERS = 64
NTYPE = 32
COL = ("col_0", "col_1", "col_2")
COL_LEV = ("col_0", "col_1", "col_2", "lev")
GROUPS = 4
CORES = 2
LANES = 128
ROWS = 8
QUARTER = 256
F32 = jnp.float32
BF16 = jnp.bfloat16
VMEM = pl.BlockSpec(memory_space=pltpu.VMEM)
SMEM = pl.BlockSpec(memory_space=pltpu.SMEM)
ANY = pl.BlockSpec(memory_space=pl.ANY)


def near(x):
    return pltpu.with_memory_space_constraint(x, pltpu.VMEM)


def halves(x, axis):
    hi = x.astype(BF16)
    lo = (x - hi.astype(F32)).astype(BF16)
    return jnp.concatenate([hi, lo], axis=axis)


def pack_kernel(lev, state, error, anom, innovation, live, kind, *refs):
    outs, (s_buf, e_buf, a_buf, m_buf, sems) = refs[:GROUPS], refs[GROUPS:]
    levels = state.shape[0]
    order = (2, 3, 1, 0)
    starts = [pl.multiple_of((lev[0] ^ d) * QUARTER, QUARTER) for d in range(GROUPS)]
    small = [
        pltpu.make_async_copy(error, e_buf, sems.at[0]),
        pltpu.make_async_copy(anom, a_buf, sems.at[1]),
        pltpu.make_async_copy(innovation, m_buf.at[0], sems.at[2]),
    ]
    parts = [
        pltpu.make_async_copy(state.at[:, :, pl.ds(starts[d], QUARTER)], s_buf.at[d], sems.at[3 + d])
        for d in range(GROUPS)
    ]
    small[0].start()
    parts[order[0]].start()
    small[1].start()
    small[2].start()
    for d in order[1:]:
        parts[d].start()
    small[1].wait()
    small[2].wait()
    rows = anom.shape[0]
    factor = m_buf[0] * live[...].astype(F32) / (MEMBERS - 1.0)
    upper = factor.astype(BF16).astype(F32)
    meta = jnp.concatenate(
        [upper, factor - upper, kind[...].astype(F32), jnp.zeros_like(factor)], axis=0
    ).astype(BF16)
    meta = jnp.concatenate([meta, jnp.zeros_like(meta)], axis=1)
    for out in outs:
        for chunk in range(anom.shape[1] // QUARTER):
            at = 2 * MEMBERS + chunk * rows
            out[at : at + rows, :] = a_buf[:, chunk * QUARTER : (chunk + 1) * QUARTER]
        out[4 * MEMBERS : 4 * MEMBERS + 16, :] = meta
    small[0].wait()
    for d in order:
        parts[d].wait()
        scale = e_buf[:, pl.ds(starts[d], QUARTER)]
        total = s_buf[d, 0].astype(F32) * scale[0:1]
        for level in range(1, levels):
            total += s_buf[d, level].astype(F32) * scale[level : level + 1]
        outs[d][0 : 2 * MEMBERS, :] = halves(total, 0)


def pack(lev, state, error, anom, innovation, live, kind):
    levels = state.shape[0]
    return pl.pallas_call(
        pack_kernel,
        in_specs=[SMEM, ANY, ANY, ANY, ANY, VMEM, VMEM],
        out_specs=[VMEM] * GROUPS,
        out_shape=[pltpu.VMEM((4 * MEMBERS + 16, QUARTER), BF16)] * GROUPS,
        scratch_shapes=[
            pltpu.VMEM((GROUPS, levels, MEMBERS, QUARTER), BF16),
            pltpu.VMEM(error.shape, F32),
            pltpu.VMEM(anom.shape, BF16),
            pltpu.VMEM((1,) + innovation.shape, F32),
            pltpu.SemaphoreType.DMA((3 + GROUPS,)),
        ],
        name="pack",
    )(lev, state, error, anom, innovation, live, kind)


def total_kernel(lev, *refs):
    parts, out, held = refs[:GROUPS], refs[GROUPS], refs[GROUPS + 1]
    half = MEMBERS
    total = parts[0][0:half, :].astype(F32) + parts[0][half : 2 * half, :].astype(F32)
    for part in parts[1:]:
        total += part[0:half, :].astype(F32) + part[half : 2 * half, :].astype(F32)
    held[...] = total
    rows = MEMBERS // GROUPS
    total = jnp.concatenate(
        [held[pl.ds(pl.multiple_of((lev[0] ^ d) * rows, rows), rows), :] for d in range(GROUPS)],
        axis=0,
    )
    out[...] = halves(total.T, 1)


def total_sens(lev, parts):
    return pl.pallas_call(
        total_kernel,
        in_specs=[SMEM] + [VMEM] * GROUPS,
        out_specs=VMEM,
        out_shape=pltpu.VMEM((QUARTER, 2 * MEMBERS), BF16),
        scratch_shapes=[pltpu.VMEM((MEMBERS, QUARTER), F32)],
        name="total",
    )(lev, *parts)


def choose(rows, bits):
    for bit in bits:
        rows = [jnp.where(bit, rows[i + 1], rows[i]) for i in range(0, len(rows), 2)]
    return rows[0]


def fill(chunk, tables, parts, spread):
    at = pl.multiple_of(2 * MEMBERS + chunk * 16, 16)
    anom = jnp.concatenate([part[pl.ds(at, 16), :] for part in parts], axis=0)
    anom = jnp.concatenate([anom, anom], axis=0)
    for side, table in enumerate(tables):
        spread[side * QUARTER : (side + 1) * QUARTER, :] = jnp.dot(
            table[...], anom, preferred_element_type=F32
        )


def consume(chunk, bases, spread, index, weight, pair, first):
    for half in range(QUARTER // LANES):
        at = pl.multiple_of(chunk * QUARTER + half * LANES, LANES)
        lanes = slice(half * LANES, (half + 1) * LANES)
        acc = jnp.zeros((ROWS, LANES), F32)
        for n in range(0, index.shape[0], ROWS):
            idx = index[n : n + ROWS, pl.ds(at, LANES)]
            row = idx & (ROWS - 1)
            bits = [(idx & (ROWS << k)) != 0 for k in range(5)]
            block = idx >> 8
            value = jnp.zeros((ROWS, LANES), F32)
            for side, base in enumerate(bases):
                got = [
                    jnp.take_along_axis(
                        spread[side * QUARTER + v * ROWS : side * QUARTER + (v + 1) * ROWS, lanes],
                        row,
                        axis=0,
                        mode="promise_in_bounds",
                    )
                    for v in range(QUARTER // ROWS)
                ]
                value = jnp.where(block == base, choose(got, bits), value)
            acc += value * weight[n : n + ROWS, pl.ds(at, LANES)]
        total = jnp.sum(acc, axis=0, keepdims=True)
        tile = chunk * (QUARTER // LANES) + half
        line = (tile >> 2) * ROWS + (tile & 3)
        pair[pl.ds(line, 1), :] = total if first is None else first[pl.ds(line, 1), :] + total


def pick(bases, tables, parts, index, weight, pair, first, even, odd):
    chunks = index.shape[1] // QUARTER
    fill(0, tables, parts, even)

    @pl.loop(0, chunks // 2)
    def _(step):
        fill(2 * step + 1, tables, parts, odd)
        consume(2 * step, bases, even, index, weight, pair, first)
        fill(jnp.minimum(2 * step + 2, chunks - 1), tables, parts, even)
        consume(2 * step + 1, bases, odd, index, weight, pair, first)


def near_kernel(lev, core, mid, mate, *refs):
    parts, (index, weight, out, even, odd) = refs[:GROUPS], refs[GROUPS:]
    group = lev[0]
    side = jnp.where(core[0] == 0, 2, 0)
    bases = (GROUPS + group, side * GROUPS + group)
    pick(bases, (mid, mate), parts, index, weight, out, None, even, odd)


def far_kernel(lev, core, far, *refs):
    parts, (index, weight, first, out, even, odd, pair) = refs[:GROUPS], refs[GROUPS:]
    group = lev[0]
    side = jnp.where(core[0] == 0, 0, 2)
    pick((side * GROUPS + group,), (far,), parts, index, weight, pair, first, even, odd)
    kinds = lax.broadcasted_iota(jnp.int32, (NTYPE, LANES), 0).astype(F32)
    sums = jnp.zeros((NTYPE, LANES), F32)
    per = ROWS // 2
    for d, part in enumerate(parts):
        meta = part[4 * MEMBERS : 4 * MEMBERS + 16, 0:LANES].astype(F32)
        share = pair[pl.ds(pl.multiple_of((group ^ d) * ROWS, ROWS), ROWS), :][0:per]
        share = share * (meta[0:per] + meta[per : 2 * per])
        for r in range(per):
            same = meta[2 * per + r : 2 * per + r + 1] == kinds
            sums += jnp.where(same, share[r : r + 1], 0.0)
    sums = jnp.sum(sums.T, axis=0, keepdims=True)
    tail = jnp.concatenate([sums, jnp.zeros((1, LANES - NTYPE), F32)], axis=1)
    tail = jnp.concatenate([tail, jnp.zeros((ROWS - per - 1, LANES), F32)], axis=0)
    for c in range(CORES):
        for g in range(GROUPS):
            mine = pair[g * ROWS : g * ROWS + per, :]
            to = c * GROUPS + g
            out[to, 0:per, :] = jnp.where(core[0] == c, mine, 0.0)
            out[to, per:ROWS, :] = tail


def finish_kernel(got, innovation, live, impact, spread):
    lines = innovation.shape[0]
    total = got[0]
    for peer in range(1, got.shape[0]):
        total += got[peer]
    pair = total[0:lines, :]
    impact[...] = pair * innovation[...] * live[...].astype(F32) / (MEMBERS - 1.0)
    for chip in range(spread.shape[0]):
        spread[chip] = total[lines : lines + 1, :]


def last_kernel(sums, impact, impact_out, type_out):
    total = sums[0]
    for chip in range(1, sums.shape[0]):
        total += sums[chip]
    type_out[...] = total[:, 0:NTYPE]
    impact_out[...] = impact[...]


def shards(state_anom, error_sum, obs_anom, local_weight, neighbours, innovation, obs_type, live):
    lines = innovation.shape[0] // LANES
    lev = lax.axis_index("lev").reshape(1)
    core = lax.axis_index("col_2").reshape(1)
    send = pack(
        lev,
        state_anom,
        error_sum,
        obs_anom,
        innovation.reshape(lines, LANES),
        live.reshape(lines, LANES),
        obs_type.reshape(lines, LANES),
    )
    parts = [send[0], None, None, None]
    for d in (2, 3, 1):
        parts[d] = lax.ppermute(send[d], "lev", [(i, i ^ d) for i in range(GROUPS)])
    parts = [near(part) for part in parts]
    mid = total_sens(lev, parts)
    pairs = lax.axis_size(COL) // CORES
    odd_even = [(CORES * i + 1, CORES * i + 2) for i in range(pairs - 1)]
    mate = lax.ppermute(mid, "col_2", [(0, 1), (1, 0)])
    far = lax.ppermute(mid, COL, odd_even + [(b, a) for a, b in odd_even])
    index, weight = near(neighbours), near(local_weight)
    lists = GROUPS * ROWS
    cost = functools.partial(pl.CostEstimate, bytes_accessed=1 << 20, transcendentals=0)
    first = pl.pallas_call(
        near_kernel,
        in_specs=[SMEM, SMEM] + [VMEM] * (GROUPS + 4),
        out_specs=VMEM,
        out_shape=pltpu.VMEM((lists, LANES), F32),
        scratch_shapes=[pltpu.VMEM((2 * QUARTER, QUARTER), F32)] * 2,
        cost_estimate=cost(flops=1 << 27),
        name="near",
    )(lev, core, near(mid), near(mate), *parts, index, weight)
    share = pl.pallas_call(
        far_kernel,
        in_specs=[SMEM, SMEM] + [VMEM] * (GROUPS + 4),
        out_specs=VMEM,
        out_shape=pltpu.VMEM((CORES * GROUPS, ROWS, LANES), F32),
        scratch_shapes=[pltpu.VMEM((QUARTER, QUARTER), F32)] * 2 + [pltpu.VMEM((lists, LANES), F32)],
        cost_estimate=cost(flops=1 << 26),
        name="far",
    )(lev, core, near(far), *parts, index, weight, near(first))
    got = lax.all_to_all(share, ("col_2", "lev"), 0, 0, tiled=True)
    chips = ("col_0", "col_1")
    impact, spread = pl.pallas_call(
        finish_kernel,
        in_specs=[VMEM] * 3,
        out_specs=[VMEM] * 2,
        out_shape=[
            pltpu.VMEM((lines, LANES), F32),
            pltpu.VMEM((lax.axis_size(chips), 1, LANES), F32),
        ],
        name="finish",
    )(near(got), near(innovation.reshape(lines, LANES)), near(live.reshape(lines, LANES)))
    sums = lax.all_to_all(spread, chips, 0, 0, tiled=True)
    impact, type_impact = pl.pallas_call(
        last_kernel,
        in_specs=[VMEM] * 2,
        out_specs=[VMEM] * 2,
        out_shape=[
            jax.ShapeDtypeStruct((lines, LANES), F32),
            jax.ShapeDtypeStruct((1, NTYPE), F32),
        ],
        name="last",
    )(near(sums), near(impact))
    return (impact.reshape(-1), type_impact.reshape(-1))


def solution(mesh):
    split = Mesh(
        mesh.devices.reshape(4, 8, 2, mesh.shape["lev"]), ("col_0", "col_1", "col_2", "lev")
    )
    return jax.shard_map(
        shards,
        mesh=split,
        in_specs=(
            P("lev", None, COL),
            P("lev", COL),
            P("lev", COL),
            P(None, COL),
            P(None, COL),
            P(COL_LEV),
            P(COL_LEV),
            P(COL_LEV),
        ),
        out_specs=(P(COL_LEV), P()),
        check_vma=False,
    )
```

```python
import functools

import jax
import jax.numpy as jnp
from jax import lax
from jax.experimental import pallas as pl
from jax.experimental.pallas import tpu as pltpu
from jax.sharding import Mesh
from jax.sharding import PartitionSpec as P

MEMBERS = 64
NTYPE = 32
COL = ("col_0", "col_1", "col_2")
COL_LEV = ("col_0", "col_1", "col_2", "lev")
GROUPS = 4
CORES = 2
LANES = 128
ROWS = 8
QUARTER = 256
F32 = jnp.float32
BF16 = jnp.bfloat16
VMEM = pl.BlockSpec(memory_space=pltpu.VMEM)
SMEM = pl.BlockSpec(memory_space=pltpu.SMEM)
ANY = pl.BlockSpec(memory_space=pl.ANY)


def near(x):
    return pltpu.with_memory_space_constraint(x, pltpu.VMEM)


def halves(x, axis):
    hi = x.astype(BF16)
    lo = (x - hi.astype(F32)).astype(BF16)
    return jnp.concatenate([hi, lo], axis=axis)


def pack_kernel(lev, state, error, innovation, live, kind, *refs):
    outs, (s_buf, e_buf, m_buf, n_buf, sems) = refs[:GROUPS], refs[GROUPS:]
    levels = state.shape[0]
    order = (1, 2, 3, 0)
    starts = [pl.multiple_of((lev[0] ^ d) * QUARTER, QUARTER) for d in range(GROUPS)]
    small = [
        pltpu.make_async_copy(error, e_buf, sems.at[0]),
        pltpu.make_async_copy(innovation, m_buf.at[0], sems.at[1]),
        pltpu.make_async_copy(live, n_buf.at[0], sems.at[2]),
        pltpu.make_async_copy(kind, n_buf.at[1], sems.at[3]),
    ]
    parts = [
        pltpu.make_async_copy(state.at[:, :, pl.ds(starts[d], QUARTER)], s_buf.at[d], sems.at[4 + d])
        for d in range(GROUPS)
    ]
    small[0].start()
    parts[order[0]].start()
    for copy in small[1:]:
        copy.start()
    for d in order[1:]:
        parts[d].start()
    for copy in small:
        copy.wait()
    factor = m_buf[0] * n_buf[0].astype(F32) / (MEMBERS - 1.0)
    upper = factor.astype(BF16).astype(F32)
    meta = jnp.concatenate(
        [upper, factor - upper, n_buf[1].astype(F32), jnp.zeros_like(factor)], axis=0
    ).astype(BF16)
    meta = jnp.concatenate([meta, jnp.zeros_like(meta)], axis=1)
    for d in order:
        parts[d].wait()
        scale = e_buf[:, pl.ds(starts[d], QUARTER)]
        total = s_buf[d, 0].astype(F32) * scale[0:1]
        for level in range(1, levels):
            total += s_buf[d, level].astype(F32) * scale[level : level + 1]
        outs[d][0 : 2 * MEMBERS, :] = halves(total, 0)
        outs[d][2 * MEMBERS :, :] = meta


def pack(lev, state, error, innovation, live, kind):
    levels = state.shape[0]
    return pl.pallas_call(
        pack_kernel,
        in_specs=[SMEM] + [ANY] * 5,
        out_specs=[VMEM] * GROUPS,
        out_shape=[pltpu.VMEM((2 * MEMBERS + 16, QUARTER), BF16)] * GROUPS,
        scratch_shapes=[
            pltpu.VMEM((GROUPS, levels, MEMBERS, QUARTER), BF16),
            pltpu.VMEM(error.shape, F32),
            pltpu.VMEM((1,) + innovation.shape, F32),
            pltpu.VMEM((2,) + live.shape, jnp.int32),
            pltpu.SemaphoreType.DMA((4 + GROUPS,)),
        ],
        name="pack",
    )(lev, state, error, innovation, live, kind)


def total_kernel(lev, *refs):
    parts, out, held = refs[:GROUPS], refs[GROUPS], refs[GROUPS + 1]
    half = MEMBERS
    total = parts[0][0:half, :].astype(F32) + parts[0][half : 2 * half, :].astype(F32)
    for part in parts[1:]:
        total += part[0:half, :].astype(F32) + part[half : 2 * half, :].astype(F32)
    held[...] = total
    rows = MEMBERS // GROUPS
    total = jnp.concatenate(
        [held[pl.ds(pl.multiple_of((lev[0] ^ d) * rows, rows), rows), :] for d in range(GROUPS)],
        axis=0,
    )
    out[...] = halves(total.T, 1)


def total_sens(lev, parts):
    return pl.pallas_call(
        total_kernel,
        in_specs=[SMEM] + [VMEM] * GROUPS,
        out_specs=VMEM,
        out_shape=pltpu.VMEM((QUARTER, 2 * MEMBERS), BF16),
        scratch_shapes=[pltpu.VMEM((MEMBERS, QUARTER), F32)],
        name="total",
    )(lev, *parts)


def choose(rows, bits):
    for bit in bits:
        rows = [jnp.where(bit, rows[i + 1], rows[i]) for i in range(0, len(rows), 2)]
    return rows[0]


def fill(chunk, tables, parts, spread):
    at = pl.multiple_of(chunk * QUARTER, QUARTER)
    anom = jnp.concatenate([part[:, pl.ds(at, QUARTER)] for part in parts], axis=0)
    anom = jnp.concatenate([anom, anom], axis=0)
    for side, table in enumerate(tables):
        spread[side * QUARTER : (side + 1) * QUARTER, :] = jnp.dot(
            table[...], anom, preferred_element_type=F32
        )


def consume(chunk, bases, spread, index, weight, pair, first):
    for half in range(QUARTER // LANES):
        at = pl.multiple_of(chunk * QUARTER + half * LANES, LANES)
        lanes = slice(half * LANES, (half + 1) * LANES)
        acc = jnp.zeros((ROWS, LANES), F32)
        for n in range(0, index.shape[0], ROWS):
            idx = index[n : n + ROWS, pl.ds(at, LANES)]
            row = idx & (ROWS - 1)
            bits = [(idx & (ROWS << k)) != 0 for k in range(5)]
            block = idx >> 8
            value = jnp.zeros((ROWS, LANES), F32)
            for side, base in enumerate(bases):
                got = [
                    jnp.take_along_axis(
                        spread[side * QUARTER + v * ROWS : side * QUARTER + (v + 1) * ROWS, lanes],
                        row,
                        axis=0,
                        mode="promise_in_bounds",
                    )
                    for v in range(QUARTER // ROWS)
                ]
                value = jnp.where(block == base, choose(got, bits), value)
            acc += value * weight[n : n + ROWS, pl.ds(at, LANES)]
        total = jnp.sum(acc, axis=0, keepdims=True)
        tile = chunk * (QUARTER // LANES) + half
        line = (tile >> 2) * ROWS + (tile & 3)
        pair[pl.ds(line, 1), :] = total if first is None else first[pl.ds(line, 1), :] + total


def pick(bases, tables, parts, index, weight, pair, first, even, odd):
    chunks = index.shape[1] // QUARTER
    fill(0, tables, parts, even)

    @pl.loop(0, chunks // 2)
    def _(step):
        fill(2 * step + 1, tables, parts, odd)
        consume(2 * step, bases, even, index, weight, pair, first)
        fill(jnp.minimum(2 * step + 2, chunks - 1), tables, parts, even)
        consume(2 * step + 1, bases, odd, index, weight, pair, first)


def near_kernel(lev, core, mid, mate, *refs):
    parts, (index, weight, out, even, odd) = refs[:GROUPS], refs[GROUPS:]
    group = lev[0]
    side = jnp.where(core[0] == 0, 2, 0)
    bases = (GROUPS + group, side * GROUPS + group)
    pick(bases, (mid, mate), parts, index, weight, out, None, even, odd)


def far_kernel(lev, core, far, *refs):
    anoms, parts = refs[:GROUPS], refs[GROUPS : 2 * GROUPS]
    index, weight, first, out, even, odd, pair = refs[2 * GROUPS :]
    group = lev[0]
    side = jnp.where(core[0] == 0, 0, 2)
    pick((side * GROUPS + group,), (far,), anoms, index, weight, pair, first, even, odd)
    kinds = lax.broadcasted_iota(jnp.int32, (NTYPE, LANES), 0).astype(F32)
    sums = jnp.zeros((NTYPE, LANES), F32)
    per = ROWS // 2
    for d, part in enumerate(parts):
        meta = part[2 * MEMBERS :, 0:LANES].astype(F32)
        share = pair[pl.ds(pl.multiple_of((group ^ d) * ROWS, ROWS), ROWS), :][0:per]
        share = share * (meta[0:per] + meta[per : 2 * per])
        for r in range(per):
            same = meta[2 * per + r : 2 * per + r + 1] == kinds
            sums += jnp.where(same, share[r : r + 1], 0.0)
    sums = jnp.sum(sums.T, axis=0, keepdims=True)
    tail = jnp.concatenate([sums, jnp.zeros((1, LANES - NTYPE), F32)], axis=1)
    tail = jnp.concatenate([tail, jnp.zeros((ROWS - per - 1, LANES), F32)], axis=0)
    for c in range(CORES):
        for g in range(GROUPS):
            mine = pair[g * ROWS : g * ROWS + per, :]
            to = c * GROUPS + g
            out[to, 0:per, :] = jnp.where(core[0] == c, mine, 0.0)
            out[to, per:ROWS, :] = tail


def finish_kernel(got, innovation, live, impact, spread):
    lines = innovation.shape[0]
    total = got[0]
    for peer in range(1, got.shape[0]):
        total += got[peer]
    pair = total[0:lines, :]
    impact[...] = pair * innovation[...] * live[...].astype(F32) / (MEMBERS - 1.0)
    for chip in range(spread.shape[0]):
        spread[chip] = total[lines : lines + 1, :]


def last_kernel(sums, impact, impact_out, type_out):
    total = sums[0]
    for chip in range(1, sums.shape[0]):
        total += sums[chip]
    type_out[...] = total[:, 0:NTYPE]
    impact_out[...] = impact[...]


def shards(state_anom, error_sum, obs_anom, local_weight, neighbours, innovation, obs_type, live):
    lines = innovation.shape[0] // LANES
    lev = lax.axis_index("lev").reshape(1)
    core = lax.axis_index("col_2").reshape(1)

    def to_groups(blocks):
        got = [
            lax.ppermute(block, "lev", [(i, i ^ d) for i in range(GROUPS)])
            for d, block in enumerate(blocks)
            if d > 0
        ]
        return [near(block) for block in [blocks[0]] + got]

    send = pack(
        lev,
        state_anom,
        error_sum,
        innovation.reshape(lines, LANES),
        live.reshape(lines, LANES),
        obs_type.reshape(lines, LANES),
    )
    parts = to_groups(send)
    anoms = to_groups([obs_anom] * GROUPS)
    mid = total_sens(lev, parts)
    pairs = lax.axis_size(COL) // CORES
    odd_even = [(CORES * i + 1, CORES * i + 2) for i in range(pairs - 1)]
    mate = lax.ppermute(mid, "col_2", [(0, 1), (1, 0)])
    far = lax.ppermute(mid, COL, odd_even + [(b, a) for a, b in odd_even])
    index, weight = near(neighbours), near(local_weight)
    lists = GROUPS * ROWS
    cost = functools.partial(pl.CostEstimate, bytes_accessed=1 << 20, transcendentals=0)
    first = pl.pallas_call(
        near_kernel,
        in_specs=[SMEM, SMEM] + [VMEM] * (GROUPS + 4),
        out_specs=VMEM,
        out_shape=pltpu.VMEM((lists, LANES), F32),
        scratch_shapes=[pltpu.VMEM((2 * QUARTER, QUARTER), F32)] * 2,
        cost_estimate=cost(flops=1 << 27),
        name="near",
    )(lev, core, near(mid), near(mate), *anoms, index, weight)
    share = pl.pallas_call(
        far_kernel,
        in_specs=[SMEM, SMEM] + [VMEM] * (2 * GROUPS + 4),
        out_specs=VMEM,
        out_shape=pltpu.VMEM((CORES * GROUPS, ROWS, LANES), F32),
        scratch_shapes=[pltpu.VMEM((QUARTER, QUARTER), F32)] * 2 + [pltpu.VMEM((lists, LANES), F32)],
        cost_estimate=cost(flops=1 << 26),
        name="far",
    )(lev, core, near(far), *anoms, *parts, index, weight, near(first))
    got = lax.all_to_all(share, ("col_2", "lev"), 0, 0, tiled=True)
    chips = ("col_0", "col_1")
    impact, spread = pl.pallas_call(
        finish_kernel,
        in_specs=[VMEM] * 3,
        out_specs=[VMEM] * 2,
        out_shape=[
            pltpu.VMEM((lines, LANES), F32),
            pltpu.VMEM((lax.axis_size(chips), 1, LANES), F32),
        ],
        name="finish",
    )(near(got), near(innovation.reshape(lines, LANES)), near(live.reshape(lines, LANES)))
    sums = lax.all_to_all(spread, chips, 0, 0, tiled=True)
    impact, type_impact = pl.pallas_call(
        last_kernel,
        in_specs=[VMEM] * 2,
        out_specs=[VMEM] * 2,
        out_shape=[
            jax.ShapeDtypeStruct((lines, LANES), F32),
            jax.ShapeDtypeStruct((1, NTYPE), F32),
        ],
        name="last",
    )(near(sums), near(impact))
    return (impact.reshape(-1), type_impact.reshape(-1))


def solution(mesh):
    split = Mesh(
        mesh.devices.reshape(4, 8, 2, mesh.shape["lev"]), ("col_0", "col_1", "col_2", "lev")
    )
    return jax.shard_map(
        shards,
        mesh=split,
        in_specs=(
            P("lev", None, COL),
            P("lev", COL),
            P("lev", COL),
            P(None, COL),
            P(None, COL),
            P(COL_LEV),
            P(COL_LEV),
            P(COL_LEV),
        ),
        out_specs=(P(COL_LEV), P()),
        check_vma=False,
    )
```

```python
import functools

import jax
import jax.numpy as jnp
from jax import lax
from jax.experimental import pallas as pl
from jax.experimental.pallas import tpu as pltpu
from jax.sharding import Mesh
from jax.sharding import PartitionSpec as P

MEMBERS = 64
NTYPE = 32
COL = ("col_0", "col_1", "col_2")
COL_LEV = ("col_0", "col_1", "col_2", "lev")
GROUPS = 4
CORES = 2
LANES = 128
ROWS = 8
QUARTER = 256
F32 = jnp.float32
BF16 = jnp.bfloat16
VMEM = pl.BlockSpec(memory_space=pltpu.VMEM)
SMEM = pl.BlockSpec(memory_space=pltpu.SMEM)
ANY = pl.BlockSpec(memory_space=pl.ANY)


def near(x):
    return pltpu.with_memory_space_constraint(x, pltpu.VMEM)


def halves(x, axis):
    hi = x.astype(BF16)
    lo = (x - hi.astype(F32)).astype(BF16)
    return jnp.concatenate([hi, lo], axis=axis)


def pack_kernel(lev, state, error, innovation, live, kind, *refs):
    outs, (s_buf, e_buf, m_buf, n_buf, sems) = refs[:GROUPS], refs[GROUPS:]
    levels = state.shape[0]
    order = (1, 2, 3, 0)
    starts = [pl.multiple_of((lev[0] ^ d) * QUARTER, QUARTER) for d in range(GROUPS)]
    small = [
        pltpu.make_async_copy(error, e_buf, sems.at[0]),
        pltpu.make_async_copy(innovation, m_buf.at[0], sems.at[1]),
        pltpu.make_async_copy(live, n_buf.at[0], sems.at[2]),
        pltpu.make_async_copy(kind, n_buf.at[1], sems.at[3]),
    ]
    parts = [
        pltpu.make_async_copy(state.at[:, :, pl.ds(starts[d], QUARTER)], s_buf.at[d], sems.at[4 + d])
        for d in range(GROUPS)
    ]
    small[0].start()
    parts[order[0]].start()
    for copy in small[1:]:
        copy.start()
    for d in order[1:]:
        parts[d].start()
    for copy in small:
        copy.wait()
    factor = m_buf[0] * n_buf[0].astype(F32) / (MEMBERS - 1.0)
    upper = factor.astype(BF16).astype(F32)
    meta = jnp.concatenate(
        [upper, factor - upper, n_buf[1].astype(F32), jnp.zeros_like(factor)], axis=0
    ).astype(BF16)
    meta = jnp.concatenate([meta, jnp.zeros_like(meta)], axis=1)
    for d in order:
        parts[d].wait()
        scale = e_buf[:, pl.ds(starts[d], QUARTER)]
        total = s_buf[d, 0].astype(F32) * scale[0:1]
        for level in range(1, levels):
            total += s_buf[d, level].astype(F32) * scale[level : level + 1]
        outs[d][0 : 2 * MEMBERS, :] = halves(total, 0)
        outs[d][2 * MEMBERS :, :] = meta


def pack(lev, state, error, innovation, live, kind):
    levels = state.shape[0]
    return pl.pallas_call(
        pack_kernel,
        in_specs=[SMEM] + [ANY] * 5,
        out_specs=[VMEM] * GROUPS,
        out_shape=[pltpu.VMEM((2 * MEMBERS + 16, QUARTER), BF16)] * GROUPS,
        scratch_shapes=[
            pltpu.VMEM((GROUPS, levels, MEMBERS, QUARTER), BF16),
            pltpu.VMEM(error.shape, F32),
            pltpu.VMEM((1,) + innovation.shape, F32),
            pltpu.VMEM((2,) + live.shape, jnp.int32),
            pltpu.SemaphoreType.DMA((4 + GROUPS,)),
        ],
        name="pack",
    )(lev, state, error, innovation, live, kind)


def total_kernel(lev, *refs):
    parts, out, held = refs[:GROUPS], refs[GROUPS], refs[GROUPS + 1]
    half = MEMBERS
    total = parts[0][0:half, :].astype(F32) + parts[0][half : 2 * half, :].astype(F32)
    for part in parts[1:]:
        total += part[0:half, :].astype(F32) + part[half : 2 * half, :].astype(F32)
    held[...] = total
    rows = MEMBERS // GROUPS
    total = jnp.concatenate(
        [held[pl.ds(pl.multiple_of((lev[0] ^ d) * rows, rows), rows), :] for d in range(GROUPS)],
        axis=0,
    )
    out[...] = halves(total.T, 1)


def total_sens(lev, parts):
    return pl.pallas_call(
        total_kernel,
        in_specs=[SMEM] + [VMEM] * GROUPS,
        out_specs=VMEM,
        out_shape=pltpu.VMEM((QUARTER, 2 * MEMBERS), BF16),
        scratch_shapes=[pltpu.VMEM((MEMBERS, QUARTER), F32)],
        name="total",
    )(lev, *parts)


def choose(rows, bits):
    for bit in bits:
        rows = [jnp.where(bit, rows[i + 1], rows[i]) for i in range(0, len(rows), 2)]
    return rows[0]


def fill(chunk, tables, parts, spread):
    at = pl.multiple_of(chunk * QUARTER, QUARTER)
    anom = jnp.concatenate([part[:, pl.ds(at, QUARTER)] for part in parts], axis=0)
    anom = jnp.concatenate([anom, anom], axis=0)
    for side, table in enumerate(tables):
        spread[side * QUARTER : (side + 1) * QUARTER, :] = jnp.dot(
            table[...], anom, preferred_element_type=F32
        )


def consume(chunk, bases, spread, index, weight, pair, first):
    for half in range(QUARTER // LANES):
        at = pl.multiple_of(chunk * QUARTER + half * LANES, LANES)
        lanes = slice(half * LANES, (half + 1) * LANES)
        acc = jnp.zeros((ROWS, LANES), F32)
        for n in range(0, index.shape[0], ROWS):
            idx = index[n : n + ROWS, pl.ds(at, LANES)]
            row = idx & (ROWS - 1)
            bits = [(idx & (ROWS << k)) != 0 for k in range(5)]
            block = idx >> 8
            value = jnp.zeros((ROWS, LANES), F32)
            for side, base in enumerate(bases):
                got = [
                    jnp.take_along_axis(
                        spread[side * QUARTER + v * ROWS : side * QUARTER + (v + 1) * ROWS, lanes],
                        row,
                        axis=0,
                        mode="promise_in_bounds",
                    )
                    for v in range(QUARTER // ROWS)
                ]
                value = jnp.where(block == base, choose(got, bits), value)
            acc += value * weight[n : n + ROWS, pl.ds(at, LANES)]
        total = jnp.sum(acc, axis=0, keepdims=True)
        tile = chunk * (QUARTER // LANES) + half
        line = (tile >> 2) * ROWS + (tile & 3)
        pair[pl.ds(line, 1), :] = total if first is None else first[pl.ds(line, 1), :] + total


def pick(bases, tables, parts, index, weight, pair, first, even, odd):
    chunks = index.shape[1] // QUARTER
    fill(0, tables, parts, even)

    @pl.loop(0, chunks // 2)
    def _(step):
        fill(2 * step + 1, tables, parts, odd)
        consume(2 * step, bases, even, index, weight, pair, first)
        fill(jnp.minimum(2 * step + 2, chunks - 1), tables, parts, even)
        consume(2 * step + 1, bases, odd, index, weight, pair, first)


def near_kernel(lev, core, mid, mate, *refs):
    parts, (index, weight, out, even, odd) = refs[:GROUPS], refs[GROUPS:]
    group = lev[0]
    side = jnp.where(core[0] == 0, 2, 0)
    bases = (GROUPS + group, side * GROUPS + group)
    pick(bases, (mid, mate), parts, index, weight, out, None, even, odd)


def far_kernel(lev, core, far, *refs):
    anoms, parts = refs[:GROUPS], refs[GROUPS : 2 * GROUPS]
    index, weight, first = refs[2 * GROUPS : 2 * GROUPS + 3]
    outs, (spread, even, odd, pair) = refs[-GROUPS - 4 : -4], refs[-4:]
    group = lev[0]
    side = jnp.where(core[0] == 0, 0, 2)
    pick((side * GROUPS + group,), (far,), anoms, index, weight, pair, first, even, odd)
    kinds = lax.broadcasted_iota(jnp.int32, (NTYPE, LANES), 0).astype(F32)
    sums = jnp.zeros((NTYPE, LANES), F32)
    per = ROWS // 2
    for d, part in enumerate(parts):
        meta = part[2 * MEMBERS :, 0:LANES].astype(F32)
        share = pair[pl.ds(pl.multiple_of((group ^ d) * ROWS, ROWS), ROWS), :][0:per]
        share = share * (meta[0:per] + meta[per : 2 * per])
        for r in range(per):
            same = meta[2 * per + r : 2 * per + r + 1] == kinds
            sums += jnp.where(same, share[r : r + 1], 0.0)
    sums = jnp.sum(sums.T, axis=0, keepdims=True)
    tail = jnp.concatenate([sums, jnp.zeros((1, LANES - NTYPE), F32)], axis=1)
    spread[...] = jnp.broadcast_to(tail[None], spread.shape)
    for d, out in enumerate(outs):
        out[...] = pair[pl.ds(pl.multiple_of((group ^ d) * ROWS, ROWS), ROWS), :]


def finish_kernel(innovation, live, *refs):
    shares, impact = refs[:-1], refs[-1]
    lines = innovation.shape[0]
    pair = shares[0][0:lines, :]
    for share in shares[1:]:
        pair += share[0:lines, :]
    impact[...] = pair * innovation[...] * live[...].astype(F32) / (MEMBERS - 1.0)


def last_kernel(sums, impact, impact_out, type_out):
    total = jnp.sum(sums[...], axis=0)
    type_out[...] = total[:, 0:NTYPE]
    impact_out[...] = impact[...]


def shards(state_anom, error_sum, obs_anom, local_weight, neighbours, innovation, obs_type, live):
    lines = innovation.shape[0] // LANES
    lev = lax.axis_index("lev").reshape(1)
    core = lax.axis_index("col_2").reshape(1)

    def to_groups(blocks):
        got = [
            lax.ppermute(block, "lev", [(i, i ^ d) for i in range(GROUPS)])
            for d, block in enumerate(blocks)
            if d > 0
        ]
        return [near(block) for block in [blocks[0]] + got]

    send = pack(
        lev,
        state_anom,
        error_sum,
        innovation.reshape(lines, LANES),
        live.reshape(lines, LANES),
        obs_type.reshape(lines, LANES),
    )
    parts = to_groups(send)
    anoms = to_groups([obs_anom] * GROUPS)
    mid = total_sens(lev, parts)
    pairs = lax.axis_size(COL) // CORES
    odd_even = [(CORES * i + 1, CORES * i + 2) for i in range(pairs - 1)]
    mate = lax.ppermute(mid, "col_2", [(0, 1), (1, 0)])
    far = lax.ppermute(mid, COL, odd_even + [(b, a) for a, b in odd_even])
    index, weight = near(neighbours), near(local_weight)
    lists = GROUPS * ROWS
    cost = functools.partial(pl.CostEstimate, bytes_accessed=1 << 20, transcendentals=0)
    first = pl.pallas_call(
        near_kernel,
        in_specs=[SMEM, SMEM] + [VMEM] * (GROUPS + 4),
        out_specs=VMEM,
        out_shape=pltpu.VMEM((lists, LANES), F32),
        scratch_shapes=[pltpu.VMEM((2 * QUARTER, QUARTER), F32)] * 2,
        cost_estimate=cost(flops=1 << 27),
        name="near",
    )(lev, core, near(mid), near(mate), *anoms, index, weight)
    everyone = lax.axis_size(COL_LEV)
    *shares, spread = pl.pallas_call(
        far_kernel,
        in_specs=[SMEM, SMEM] + [VMEM] * (2 * GROUPS + 4),
        out_specs=[VMEM] * (GROUPS + 1),
        out_shape=[pltpu.VMEM((ROWS, LANES), F32)] * GROUPS
        + [jax.ShapeDtypeStruct((everyone, 1, LANES), F32)],
        scratch_shapes=[pltpu.VMEM((QUARTER, QUARTER), F32)] * 2 + [pltpu.VMEM((lists, LANES), F32)],
        cost_estimate=cost(flops=1 << 26),
        name="far",
    )(lev, core, near(far), *anoms, *parts, index, weight, near(first))
    sums = lax.all_to_all(spread, COL_LEV, 0, 0, tiled=True)
    impact = pl.pallas_call(
        finish_kernel,
        in_specs=[VMEM] * (GROUPS + 2),
        out_specs=VMEM,
        out_shape=pltpu.VMEM((lines, LANES), F32),
        name="finish",
    )(
        near(innovation.reshape(lines, LANES)),
        near(live.reshape(lines, LANES)),
        *to_groups(shares),
    )
    impact, type_impact = pl.pallas_call(
        last_kernel,
        in_specs=[VMEM] * 2,
        out_specs=[VMEM] * 2,
        out_shape=[
            jax.ShapeDtypeStruct((lines, LANES), F32),
            jax.ShapeDtypeStruct((1, NTYPE), F32),
        ],
        name="last",
    )(near(sums), near(impact))
    return (impact.reshape(-1), type_impact.reshape(-1))


def solution(mesh):
    split = Mesh(
        mesh.devices.reshape(4, 8, 2, mesh.shape["lev"]), ("col_0", "col_1", "col_2", "lev")
    )
    return jax.shard_map(
        shards,
        mesh=split,
        in_specs=(
            P("lev", None, COL),
            P("lev", COL),
            P("lev", COL),
            P(None, COL),
            P(None, COL),
            P(COL_LEV),
            P(COL_LEV),
            P(COL_LEV),
        ),
        out_specs=(P(COL_LEV), P()),
        check_vma=False,
    )
```

```python
import functools

import jax
import jax.numpy as jnp
from jax import lax
from jax.experimental import pallas as pl
from jax.experimental.pallas import tpu as pltpu
from jax.sharding import Mesh
from jax.sharding import PartitionSpec as P

MEMBERS = 64
NTYPE = 32
COL = ("col_0", "col_1", "col_2")
COL_LEV = ("col_0", "col_1", "col_2", "lev")
GROUPS = 4
CORES = 2
LANES = 128
ROWS = 8
QUARTER = 256
F32 = jnp.float32
BF16 = jnp.bfloat16
VMEM = pl.BlockSpec(memory_space=pltpu.VMEM)
SMEM = pl.BlockSpec(memory_space=pltpu.SMEM)
ANY = pl.BlockSpec(memory_space=pl.ANY)


def near(x):
    return pltpu.with_memory_space_constraint(x, pltpu.VMEM)


def halves(x, axis):
    hi = x.astype(BF16)
    lo = (x - hi.astype(F32)).astype(BF16)
    return jnp.concatenate([hi, lo], axis=axis)


def pack_kernel(lev, state, error, innovation, live, kind, *refs):
    outs, (s_buf, e_buf, m_buf, n_buf, sems) = refs[:GROUPS], refs[GROUPS:]
    levels = state.shape[0]
    order = (1, 2, 3, 0)
    starts = [pl.multiple_of((lev[0] ^ d) * QUARTER, QUARTER) for d in range(GROUPS)]
    small = [
        pltpu.make_async_copy(error, e_buf, sems.at[0]),
        pltpu.make_async_copy(innovation, m_buf.at[0], sems.at[1]),
        pltpu.make_async_copy(live, n_buf.at[0], sems.at[2]),
        pltpu.make_async_copy(kind, n_buf.at[1], sems.at[3]),
    ]
    parts = [
        pltpu.make_async_copy(state.at[:, :, pl.ds(starts[d], QUARTER)], s_buf.at[d], sems.at[4 + d])
        for d in range(GROUPS)
    ]
    small[0].start()
    parts[order[0]].start()
    for copy in small[1:]:
        copy.start()
    for d in order[1:]:
        parts[d].start()
    for copy in small:
        copy.wait()
    factor = m_buf[0] * n_buf[0].astype(F32) / (MEMBERS - 1.0)
    upper = factor.astype(BF16).astype(F32)
    meta = jnp.concatenate(
        [upper, factor - upper, n_buf[1].astype(F32), jnp.zeros_like(factor)], axis=0
    ).astype(BF16)
    meta = jnp.concatenate([meta, jnp.zeros_like(meta)], axis=1)
    for d in order:
        parts[d].wait()
        scale = e_buf[:, pl.ds(starts[d], QUARTER)]
        total = s_buf[d, 0].astype(F32) * scale[0:1]
        for level in range(1, levels):
            total += s_buf[d, level].astype(F32) * scale[level : level + 1]
        outs[d][0 : 2 * MEMBERS, :] = halves(total, 0)
        outs[d][2 * MEMBERS :, :] = meta


def pack(lev, state, error, innovation, live, kind):
    levels = state.shape[0]
    return pl.pallas_call(
        pack_kernel,
        in_specs=[SMEM] + [ANY] * 5,
        out_specs=[VMEM] * GROUPS,
        out_shape=[pltpu.VMEM((2 * MEMBERS + 16, QUARTER), BF16)] * GROUPS,
        scratch_shapes=[
            pltpu.VMEM((GROUPS, levels, MEMBERS, QUARTER), BF16),
            pltpu.VMEM(error.shape, F32),
            pltpu.VMEM((1,) + innovation.shape, F32),
            pltpu.VMEM((2,) + live.shape, jnp.int32),
            pltpu.SemaphoreType.DMA((4 + GROUPS,)),
        ],
        name="pack",
    )(lev, state, error, innovation, live, kind)


def total_kernel(lev, *refs):
    parts, out, held = refs[:GROUPS], refs[GROUPS], refs[GROUPS + 1]
    half = MEMBERS
    total = parts[0][0:half, :].astype(F32) + parts[0][half : 2 * half, :].astype(F32)
    for part in parts[1:]:
        total += part[0:half, :].astype(F32) + part[half : 2 * half, :].astype(F32)
    held[...] = total
    rows = MEMBERS // GROUPS
    total = jnp.concatenate(
        [held[pl.ds(pl.multiple_of((lev[0] ^ d) * rows, rows), rows), :] for d in range(GROUPS)],
        axis=0,
    )
    out[...] = halves(total.T, 1)


def total_sens(lev, parts):
    return pl.pallas_call(
        total_kernel,
        in_specs=[SMEM] + [VMEM] * GROUPS,
        out_specs=VMEM,
        out_shape=pltpu.VMEM((QUARTER, 2 * MEMBERS), BF16),
        scratch_shapes=[pltpu.VMEM((MEMBERS, QUARTER), F32)],
        name="total",
    )(lev, *parts)


def choose(rows, bits):
    for bit in bits:
        rows = [jnp.where(bit, rows[i + 1], rows[i]) for i in range(0, len(rows), 2)]
    return rows[0]


def fill(chunk, tables, parts, spread):
    at = pl.multiple_of(chunk * QUARTER, QUARTER)
    anom = jnp.concatenate([part[:, pl.ds(at, QUARTER)] for part in parts], axis=0)
    anom = jnp.concatenate([anom, anom], axis=0)
    for side, table in enumerate(tables):
        spread[side * QUARTER : (side + 1) * QUARTER, :] = jnp.dot(
            table[...], anom, preferred_element_type=F32
        )


def consume(chunk, bases, spread, index, weight, pair, first):
    for half in range(QUARTER // LANES):
        at = pl.multiple_of(chunk * QUARTER + half * LANES, LANES)
        lanes = slice(half * LANES, (half + 1) * LANES)
        acc = jnp.zeros((ROWS, LANES), F32)
        for n in range(0, index.shape[0], ROWS):
            idx = index[n : n + ROWS, pl.ds(at, LANES)]
            row = idx & (ROWS - 1)
            bits = [(idx & (ROWS << k)) != 0 for k in range(5)]
            block = idx >> 8
            value = jnp.zeros((ROWS, LANES), F32)
            for side, base in enumerate(bases):
                got = [
                    jnp.take_along_axis(
                        spread[side * QUARTER + v * ROWS : side * QUARTER + (v + 1) * ROWS, lanes],
                        row,
                        axis=0,
                        mode="promise_in_bounds",
                    )
                    for v in range(QUARTER // ROWS)
                ]
                value = jnp.where(block == base, choose(got, bits), value)
            acc += value * weight[n : n + ROWS, pl.ds(at, LANES)]
        total = jnp.sum(acc, axis=0, keepdims=True)
        tile = chunk * (QUARTER // LANES) + half
        line = (tile >> 2) * ROWS + (tile & 3)
        pair[pl.ds(line, 1), :] = total if first is None else first[pl.ds(line, 1), :] + total


def pick(bases, tables, parts, index, weight, pair, first, even, odd):
    chunks = index.shape[1] // QUARTER
    fill(0, tables, parts, even)

    @pl.loop(0, chunks // 2)
    def _(step):
        fill(2 * step + 1, tables, parts, odd)
        consume(2 * step, bases, even, index, weight, pair, first)
        fill(jnp.minimum(2 * step + 2, chunks - 1), tables, parts, even)
        consume(2 * step + 1, bases, odd, index, weight, pair, first)


def near_kernel(lev, core, mid, mate, *refs):
    parts, (index, weight, out, even, odd) = refs[:GROUPS], refs[GROUPS:]
    group = lev[0]
    side = jnp.where(core[0] == 0, 2, 0)
    bases = (GROUPS + group, side * GROUPS + group)
    pick(bases, (mid, mate), parts, index, weight, out, None, even, odd)


def far_kernel(lev, core, far, *refs):
    anoms, parts = refs[:GROUPS], refs[GROUPS : 2 * GROUPS]
    index, weight, first = refs[2 * GROUPS : 2 * GROUPS + 3]
    outs, (spread, even, odd, pair) = refs[-GROUPS - 4 : -4], refs[-4:]
    group = lev[0]
    side = jnp.where(core[0] == 0, 0, 2)
    pick((side * GROUPS + group,), (far,), anoms, index, weight, pair, first, even, odd)
    kinds = lax.broadcasted_iota(jnp.int32, (NTYPE, LANES), 0).astype(F32)
    sums = jnp.zeros((NTYPE, LANES), F32)
    per = ROWS // 2
    for d, part in enumerate(parts):
        meta = part[2 * MEMBERS :, 0:LANES].astype(F32)
        share = pair[pl.ds(pl.multiple_of((group ^ d) * ROWS, ROWS), ROWS), :][0:per]
        share = share * (meta[0:per] + meta[per : 2 * per])
        for r in range(per):
            same = meta[2 * per + r : 2 * per + r + 1] == kinds
            sums += jnp.where(same, share[r : r + 1], 0.0)
    sums = jnp.sum(sums.T, axis=0, keepdims=True)
    tail = jnp.concatenate([sums, jnp.zeros((1, LANES - NTYPE), F32)], axis=1)
    spread[...] = jnp.broadcast_to(tail[None], spread.shape)
    for d, out in enumerate(outs):
        out[...] = pair[pl.ds(pl.multiple_of((group ^ d) * ROWS, ROWS), ROWS), :]


def finish_kernel(innovation, live, *refs):
    shares, impact = refs[:-1], refs[-1]
    lines = innovation.shape[0]
    pair = shares[0][0:lines, :]
    for share in shares[1:]:
        pair += share[0:lines, :]
    impact[...] = pair * innovation[...] * live[...].astype(F32) / (MEMBERS - 1.0)


def last_kernel(sums, impact, impact_out, type_out):
    total = jnp.sum(sums[...], axis=0)
    type_out[...] = total[:, 0:NTYPE]
    impact_out[...] = impact[...]


def steps(state_anom, error_sum, obs_anom, local_weight, neighbours, innovation, obs_type, live):
    lines = innovation.shape[0] // LANES
    lev = lax.axis_index("lev").reshape(1)
    core = lax.axis_index("col_2").reshape(1)

    def to_groups(blocks):
        got = [blocks[0]]
        for d in range(1, GROUPS):
            got.append(lax.ppermute(blocks[d], "lev", [(i, i ^ d) for i in range(GROUPS)]))
        return [near(block) for block in got]

    send = pack(
        lev,
        state_anom,
        error_sum,
        innovation.reshape(lines, LANES),
        live.reshape(lines, LANES),
        obs_type.reshape(lines, LANES),
    )
    parts = to_groups(send)
    anoms = to_groups([obs_anom] * GROUPS)
    mid = total_sens(lev, parts)
    pairs = lax.axis_size(COL) // CORES
    odd_even = [(CORES * i + 1, CORES * i + 2) for i in range(pairs - 1)]
    far = lax.ppermute(mid, COL, odd_even + [(b, a) for a, b in odd_even])
    mate = lax.ppermute(mid, "col_2", [(0, 1), (1, 0)])
    index, weight = near(neighbours), near(local_weight)
    lists = GROUPS * ROWS
    cost = functools.partial(pl.CostEstimate, bytes_accessed=1 << 20, transcendentals=0)
    first = pl.pallas_call(
        near_kernel,
        in_specs=[SMEM, SMEM] + [VMEM] * (GROUPS + 4),
        out_specs=VMEM,
        out_shape=pltpu.VMEM((lists, LANES), F32),
        scratch_shapes=[pltpu.VMEM((2 * QUARTER, QUARTER), F32)] * 2,
        cost_estimate=cost(flops=1 << 27),
        name="near",
    )(lev, core, near(mid), near(mate), *anoms, index, weight)
    everyone = lax.axis_size(COL_LEV)
    *shares, spread = pl.pallas_call(
        far_kernel,
        in_specs=[SMEM, SMEM] + [VMEM] * (2 * GROUPS + 4),
        out_specs=[VMEM] * (GROUPS + 1),
        out_shape=[pltpu.VMEM((ROWS, LANES), F32)] * GROUPS
        + [jax.ShapeDtypeStruct((everyone, 1, LANES), F32)],
        scratch_shapes=[pltpu.VMEM((QUARTER, QUARTER), F32)] * 2 + [pltpu.VMEM((lists, LANES), F32)],
        cost_estimate=cost(flops=1 << 26),
        name="far",
    )(lev, core, near(far), *anoms, *parts, index, weight, near(first))
    sums = lax.all_to_all(spread, COL_LEV, 0, 0, tiled=True)
    impact = pl.pallas_call(
        finish_kernel,
        in_specs=[VMEM] * (GROUPS + 2),
        out_specs=VMEM,
        out_shape=pltpu.VMEM((lines, LANES), F32),
        name="finish",
    )(
        near(innovation.reshape(lines, LANES)),
        near(live.reshape(lines, LANES)),
        *to_groups(shares),
    )
    impact, type_impact = pl.pallas_call(
        last_kernel,
        in_specs=[VMEM] * 2,
        out_specs=[VMEM] * 2,
        out_shape=[
            jax.ShapeDtypeStruct((lines, LANES), F32),
            jax.ShapeDtypeStruct((1, NTYPE), F32),
        ],
        name="last",
    )(near(sums), near(impact))
    return (impact.reshape(-1), type_impact.reshape(-1))


def solution(mesh):
    split = Mesh(
        mesh.devices.reshape(4, 8, 2, mesh.shape["lev"]), ("col_0", "col_1", "col_2", "lev")
    )
    return jax.shard_map(
        steps,
        mesh=split,
        in_specs=(
            P("lev", None, COL),
            P("lev", COL),
            P("lev", COL),
            P(None, COL),
            P(None, COL),
            P(COL_LEV),
            P(COL_LEV),
            P(COL_LEV),
        ),
        out_specs=(P(COL_LEV), P()),
        check_vma=False,
    )
```

```python
import functools

import jax
import jax.numpy as jnp
from jax import lax
from jax.experimental import pallas as pl
from jax.experimental.pallas import tpu as pltpu
from jax.sharding import Mesh
from jax.sharding import PartitionSpec as P

MEMBERS = 64
NTYPE = 32
COL = ("col_0", "col_1", "col_2")
COL_LEV = ("col_0", "col_1", "col_2", "lev")
GROUPS = 4
CORES = 2
LANES = 128
ROWS = 8
QUARTER = 256
F32 = jnp.float32
BF16 = jnp.bfloat16
VMEM = pl.BlockSpec(memory_space=pltpu.VMEM)
SMEM = pl.BlockSpec(memory_space=pltpu.SMEM)
ANY = pl.BlockSpec(memory_space=pl.ANY)


def near(x):
    return pltpu.with_memory_space_constraint(x, pltpu.VMEM)


def halves(x, axis):
    hi = x.astype(BF16)
    lo = (x - hi.astype(F32)).astype(BF16)
    return jnp.concatenate([hi, lo], axis=axis)


def pack_kernel(lev, state, error, innovation, live, kind, *refs):
    outs, (s_buf, e_buf, m_buf, n_buf, sems) = refs[:GROUPS], refs[GROUPS:]
    levels = state.shape[0]
    order = (1, 2, 3, 0)
    starts = [pl.multiple_of((lev[0] ^ d) * QUARTER, QUARTER) for d in range(GROUPS)]
    small = [
        pltpu.make_async_copy(error, e_buf, sems.at[0]),
        pltpu.make_async_copy(innovation, m_buf.at[0], sems.at[1]),
        pltpu.make_async_copy(live, n_buf.at[0], sems.at[2]),
        pltpu.make_async_copy(kind, n_buf.at[1], sems.at[3]),
    ]
    parts = [
        pltpu.make_async_copy(state.at[:, :, pl.ds(starts[d], QUARTER)], s_buf.at[d], sems.at[4 + d])
        for d in range(GROUPS)
    ]
    small[0].start()
    parts[order[0]].start()
    for copy in small[1:]:
        copy.start()
    for d in order[1:]:
        parts[d].start()
    for copy in small:
        copy.wait()
    factor = m_buf[0] * n_buf[0].astype(F32) / (MEMBERS - 1.0)
    upper = factor.astype(BF16).astype(F32)
    meta = jnp.concatenate(
        [upper, factor - upper, n_buf[1].astype(F32), jnp.zeros_like(factor)], axis=0
    ).astype(BF16)
    meta = jnp.concatenate([meta, jnp.zeros_like(meta)], axis=1)
    for d in order:
        parts[d].wait()
        scale = e_buf[:, pl.ds(starts[d], QUARTER)]
        total = s_buf[d, 0].astype(F32) * scale[0:1]
        for level in range(1, levels):
            total += s_buf[d, level].astype(F32) * scale[level : level + 1]
        outs[d][0 : 2 * MEMBERS, :] = halves(total, 0)
        outs[d][2 * MEMBERS :, :] = meta


def pack(lev, state, error, innovation, live, kind):
    levels = state.shape[0]
    return pl.pallas_call(
        pack_kernel,
        in_specs=[SMEM] + [ANY] * 5,
        out_specs=[VMEM] * GROUPS,
        out_shape=[pltpu.VMEM((2 * MEMBERS + 16, QUARTER), BF16)] * GROUPS,
        scratch_shapes=[
            pltpu.VMEM((GROUPS, levels, MEMBERS, QUARTER), BF16),
            pltpu.VMEM(error.shape, F32),
            pltpu.VMEM((1,) + innovation.shape, F32),
            pltpu.VMEM((2,) + live.shape, jnp.int32),
            pltpu.SemaphoreType.DMA((4 + GROUPS,)),
        ],
        name="pack",
    )(lev, state, error, innovation, live, kind)


def total_kernel(lev, *refs):
    parts, out, held = refs[:GROUPS], refs[GROUPS], refs[GROUPS + 1]
    half = MEMBERS
    total = parts[0][0:half, :].astype(F32) + parts[0][half : 2 * half, :].astype(F32)
    for part in parts[1:]:
        total += part[0:half, :].astype(F32) + part[half : 2 * half, :].astype(F32)
    held[...] = total
    rows = MEMBERS // GROUPS
    total = jnp.concatenate(
        [held[pl.ds(pl.multiple_of((lev[0] ^ d) * rows, rows), rows), :] for d in range(GROUPS)],
        axis=0,
    )
    out[...] = halves(total.T, 1)


def total_sens(lev, parts):
    return pl.pallas_call(
        total_kernel,
        in_specs=[SMEM] + [VMEM] * GROUPS,
        out_specs=VMEM,
        out_shape=pltpu.VMEM((QUARTER, 2 * MEMBERS), BF16),
        scratch_shapes=[pltpu.VMEM((MEMBERS, QUARTER), F32)],
        name="total",
    )(lev, *parts)


def choose(got, bits, low, depth):
    if depth == 0:
        return got(low)
    upper = choose(got, bits, low + (1 << (depth - 1)), depth - 1)
    return jnp.where(bits[depth - 1], upper, choose(got, bits, low, depth - 1))


def fill(chunk, tables, parts, spread):
    at = pl.multiple_of(chunk * QUARTER, QUARTER)
    anom = jnp.concatenate([part[:, pl.ds(at, QUARTER)] for part in parts], axis=0)
    anom = jnp.concatenate([anom, anom], axis=0)
    for side, table in enumerate(tables):
        spread[side * QUARTER : (side + 1) * QUARTER, :] = jnp.dot(
            table[...], anom, preferred_element_type=F32
        )


def consume(chunk, bases, spread, index, weight, pair, first):
    for half in range(QUARTER // LANES):
        at = pl.multiple_of(chunk * QUARTER + half * LANES, LANES)
        lanes = slice(half * LANES, (half + 1) * LANES)
        acc = jnp.zeros((ROWS, LANES), F32)
        for n in range(0, index.shape[0], ROWS):
            idx = index[n : n + ROWS, pl.ds(at, LANES)]
            row = idx & (ROWS - 1)
            bits = [(idx & (ROWS << k)) != 0 for k in range(5)]
            block = idx >> 8
            value = jnp.zeros((ROWS, LANES), F32)
            for side, base in enumerate(bases):

                def got(v):
                    at_row = side * QUARTER + v * ROWS
                    return jnp.take_along_axis(
                        spread[at_row : at_row + ROWS, lanes], row, axis=0, mode="promise_in_bounds"
                    )

                value = jnp.where(block == base, choose(got, bits, 0, len(bits)), value)
            acc += value * weight[n : n + ROWS, pl.ds(at, LANES)]
        total = jnp.sum(acc, axis=0, keepdims=True)
        tile = chunk * (QUARTER // LANES) + half
        line = (tile >> 2) * ROWS + (tile & 3)
        pair[pl.ds(line, 1), :] = total if first is None else first[pl.ds(line, 1), :] + total


def pick(bases, tables, parts, index, weight, pair, first, even, odd):
    chunks = index.shape[1] // QUARTER
    slots = [even, odd]
    fill(0, tables, parts, even)
    for chunk in range(chunks):
        if chunk + 1 < chunks:
            fill(chunk + 1, tables, parts, slots[(chunk + 1) % 2])
        consume(chunk, bases, slots[chunk % 2], index, weight, pair, first)


def near_kernel(lev, core, mid, mate, *refs):
    parts, (index, weight, out, even, odd) = refs[:GROUPS], refs[GROUPS:]
    group = lev[0]
    side = jnp.where(core[0] == 0, 2, 0)
    bases = (GROUPS + group, side * GROUPS + group)
    pick(bases, (mid, mate), parts, index, weight, out, None, even, odd)


def far_kernel(lev, core, far, *refs):
    anoms, parts = refs[:GROUPS], refs[GROUPS : 2 * GROUPS]
    index, weight, first = refs[2 * GROUPS : 2 * GROUPS + 3]
    outs, (spread, even, odd, pair) = refs[-GROUPS - 4 : -4], refs[-4:]
    group = lev[0]
    side = jnp.where(core[0] == 0, 0, 2)
    pick((side * GROUPS + group,), (far,), anoms, index, weight, pair, first, even, odd)
    kinds = lax.broadcasted_iota(jnp.int32, (NTYPE, LANES), 0).astype(F32)
    sums = jnp.zeros((NTYPE, LANES), F32)
    per = ROWS // 2
    for d, part in enumerate(parts):
        meta = part[2 * MEMBERS :, 0:LANES].astype(F32)
        share = pair[pl.ds(pl.multiple_of((group ^ d) * ROWS, ROWS), ROWS), :][0:per]
        share = share * (meta[0:per] + meta[per : 2 * per])
        for r in range(per):
            same = meta[2 * per + r : 2 * per + r + 1] == kinds
            sums += jnp.where(same, share[r : r + 1], 0.0)
    sums = jnp.sum(sums.T, axis=0, keepdims=True)
    tail = jnp.concatenate([sums, jnp.zeros((1, LANES - NTYPE), F32)], axis=1)
    spread[...] = jnp.broadcast_to(tail[None], spread.shape)
    for d, out in enumerate(outs):
        out[...] = pair[pl.ds(pl.multiple_of((group ^ d) * ROWS, ROWS), ROWS), :]


def finish_kernel(innovation, live, *refs):
    shares, impact = refs[:-1], refs[-1]
    lines = innovation.shape[0]
    pair = shares[0][0:lines, :]
    for share in shares[1:]:
        pair += share[0:lines, :]
    impact[...] = pair * innovation[...] * live[...].astype(F32) / (MEMBERS - 1.0)


def last_kernel(sums, impact, impact_out, type_out):
    total = jnp.sum(sums[...], axis=0)
    type_out[...] = total[:, 0:NTYPE]
    impact_out[...] = impact[...]


def shards(state_anom, error_sum, obs_anom, local_weight, neighbours, innovation, obs_type, live):
    lines = innovation.shape[0] // LANES
    lev = lax.axis_index("lev").reshape(1)
    core = lax.axis_index("col_2").reshape(1)

    def to_groups(blocks):
        got = [
            lax.ppermute(block, "lev", [(i, i ^ d) for i in range(GROUPS)])
            for d, block in enumerate(blocks)
            if d > 0
        ]
        return [near(block) for block in [blocks[0]] + got]

    send = pack(
        lev,
        state_anom,
        error_sum,
        innovation.reshape(lines, LANES),
        live.reshape(lines, LANES),
        obs_type.reshape(lines, LANES),
    )
    parts = to_groups(send)
    anoms = to_groups([obs_anom] * GROUPS)
    mid = total_sens(lev, parts)
    pairs = lax.axis_size(COL) // CORES
    odd_even = [(CORES * i + 1, CORES * i + 2) for i in range(pairs - 1)]
    mate = lax.ppermute(mid, "col_2", [(0, 1), (1, 0)])
    far = lax.ppermute(mid, COL, odd_even + [(b, a) for a, b in odd_even])
    index, weight = near(neighbours), near(local_weight)
    lists = GROUPS * ROWS
    cost = functools.partial(pl.CostEstimate, bytes_accessed=1 << 20, transcendentals=0)
    first = pl.pallas_call(
        near_kernel,
        in_specs=[SMEM, SMEM] + [VMEM] * (GROUPS + 4),
        out_specs=VMEM,
        out_shape=pltpu.VMEM((lists, LANES), F32),
        scratch_shapes=[pltpu.VMEM((2 * QUARTER, QUARTER), F32)] * 2,
        cost_estimate=cost(flops=1 << 27),
        name="near",
    )(lev, core, near(mid), near(mate), *anoms, index, weight)
    everyone = lax.axis_size(COL_LEV)
    *shares, spread = pl.pallas_call(
        far_kernel,
        in_specs=[SMEM, SMEM] + [VMEM] * (2 * GROUPS + 4),
        out_specs=[VMEM] * (GROUPS + 1),
        out_shape=[pltpu.VMEM((ROWS, LANES), F32)] * GROUPS
        + [jax.ShapeDtypeStruct((everyone, 1, LANES), F32)],
        scratch_shapes=[pltpu.VMEM((QUARTER, QUARTER), F32)] * 2 + [pltpu.VMEM((lists, LANES), F32)],
        cost_estimate=cost(flops=1 << 26),
        name="far",
    )(lev, core, near(far), *anoms, *parts, index, weight, near(first))
    sums = lax.all_to_all(spread, COL_LEV, 0, 0, tiled=True)
    impact = pl.pallas_call(
        finish_kernel,
        in_specs=[VMEM] * (GROUPS + 2),
        out_specs=VMEM,
        out_shape=pltpu.VMEM((lines, LANES), F32),
        name="finish",
    )(
        near(innovation.reshape(lines, LANES)),
        near(live.reshape(lines, LANES)),
        *to_groups(shares),
    )
    impact, type_impact = pl.pallas_call(
        last_kernel,
        in_specs=[VMEM] * 2,
        out_specs=[VMEM] * 2,
        out_shape=[
            jax.ShapeDtypeStruct((lines, LANES), F32),
            jax.ShapeDtypeStruct((1, NTYPE), F32),
        ],
        name="last",
    )(near(sums), near(impact))
    return (impact.reshape(-1), type_impact.reshape(-1))


def solution(mesh):
    split = Mesh(
        mesh.devices.reshape(4, 8, 2, mesh.shape["lev"]), ("col_0", "col_1", "col_2", "lev")
    )
    return jax.shard_map(
        shards,
        mesh=split,
        in_specs=(
            P("lev", None, COL),
            P("lev", COL),
            P("lev", COL),
            P(None, COL),
            P(None, COL),
            P(COL_LEV),
            P(COL_LEV),
            P(COL_LEV),
        ),
        out_specs=(P(COL_LEV), P()),
        check_vma=False,
    )
```

```python
import functools

import jax
import jax.numpy as jnp
from jax import lax
from jax.experimental import pallas as pl
from jax.experimental.pallas import tpu as pltpu
from jax.sharding import Mesh
from jax.sharding import PartitionSpec as P

MEMBERS = 64
NTYPE = 32
COL = ("col_0", "col_1", "col_2")
COL_LEV = ("col_0", "col_1", "col_2", "lev")
GROUPS = 4
CORES = 2
LANES = 128
ROWS = 8
QUARTER = 256
F32 = jnp.float32
BF16 = jnp.bfloat16
VMEM = pl.BlockSpec(memory_space=pltpu.VMEM)
SMEM = pl.BlockSpec(memory_space=pltpu.SMEM)
ANY = pl.BlockSpec(memory_space=pl.ANY)


def near(x):
    return pltpu.with_memory_space_constraint(x, pltpu.VMEM)


def halves(x, axis):
    hi = x.astype(BF16)
    lo = (x - hi.astype(F32)).astype(BF16)
    return jnp.concatenate([hi, lo], axis=axis)


def pack_kernel(lev, state, error, innovation, live, kind, *refs):
    outs, (s_buf, e_buf, m_buf, n_buf, sems) = refs[:GROUPS], refs[GROUPS:]
    levels = state.shape[0]
    order = (1, 2, 3, 0)
    starts = [pl.multiple_of((lev[0] ^ d) * QUARTER, QUARTER) for d in range(GROUPS)]
    small = [
        pltpu.make_async_copy(error, e_buf, sems.at[0]),
        pltpu.make_async_copy(innovation, m_buf.at[0], sems.at[1]),
        pltpu.make_async_copy(live, n_buf.at[0], sems.at[2]),
        pltpu.make_async_copy(kind, n_buf.at[1], sems.at[3]),
    ]
    parts = [
        pltpu.make_async_copy(state.at[:, :, pl.ds(starts[d], QUARTER)], s_buf.at[d], sems.at[4 + d])
        for d in range(GROUPS)
    ]
    small[0].start()
    parts[order[0]].start()
    for copy in small[1:]:
        copy.start()
    for d in order[1:]:
        parts[d].start()
    for copy in small:
        copy.wait()
    factor = m_buf[0] * n_buf[0].astype(F32) / (MEMBERS - 1.0)
    upper = factor.astype(BF16).astype(F32)
    meta = jnp.concatenate(
        [upper, factor - upper, n_buf[1].astype(F32), jnp.zeros_like(factor)], axis=0
    ).astype(BF16)
    meta = jnp.concatenate([meta, jnp.zeros_like(meta)], axis=1)
    for d in order:
        parts[d].wait()
        scale = e_buf[:, pl.ds(starts[d], QUARTER)]
        total = s_buf[d, 0].astype(F32) * scale[0:1]
        for level in range(1, levels):
            total += s_buf[d, level].astype(F32) * scale[level : level + 1]
        outs[d][0 : 2 * MEMBERS, :] = halves(total, 0)
        outs[d][2 * MEMBERS :, :] = meta


def pack(lev, state, error, innovation, live, kind):
    levels = state.shape[0]
    return pl.pallas_call(
        pack_kernel,
        in_specs=[SMEM] + [ANY] * 5,
        out_specs=[VMEM] * GROUPS,
        out_shape=[pltpu.VMEM((2 * MEMBERS + 16, QUARTER), BF16)] * GROUPS,
        scratch_shapes=[
            pltpu.VMEM((GROUPS, levels, MEMBERS, QUARTER), BF16),
            pltpu.VMEM(error.shape, F32),
            pltpu.VMEM((1,) + innovation.shape, F32),
            pltpu.VMEM((2,) + live.shape, jnp.int32),
            pltpu.SemaphoreType.DMA((4 + GROUPS,)),
        ],
        name="pack",
    )(lev, state, error, innovation, live, kind)


def total_kernel(lev, *refs):
    parts, out, held = refs[:GROUPS], refs[GROUPS], refs[GROUPS + 1]
    half = MEMBERS
    total = parts[0][0:half, :].astype(F32) + parts[0][half : 2 * half, :].astype(F32)
    for part in parts[1:]:
        total += part[0:half, :].astype(F32) + part[half : 2 * half, :].astype(F32)
    held[...] = total
    rows = MEMBERS // GROUPS
    total = jnp.concatenate(
        [held[pl.ds(pl.multiple_of((lev[0] ^ d) * rows, rows), rows), :] for d in range(GROUPS)],
        axis=0,
    )
    out[...] = halves(total.T, 1)


def total_sens(lev, parts):
    return pl.pallas_call(
        total_kernel,
        in_specs=[SMEM] + [VMEM] * GROUPS,
        out_specs=VMEM,
        out_shape=pltpu.VMEM((QUARTER, 2 * MEMBERS), BF16),
        scratch_shapes=[pltpu.VMEM((MEMBERS, QUARTER), F32)],
        name="total",
    )(lev, *parts)


def choose(got, bits, low, depth):
    if depth == 0:
        return got(low)
    upper = choose(got, bits, low + (1 << (depth - 1)), depth - 1)
    return jnp.where(bits[depth - 1], upper, choose(got, bits, low, depth - 1))


def fill(chunk, tables, parts, spread):
    at = pl.multiple_of(chunk * QUARTER, QUARTER)
    anom = jnp.concatenate([part[:, pl.ds(at, QUARTER)] for part in parts], axis=0)
    anom = jnp.concatenate([anom, anom], axis=0)
    for side, table in enumerate(tables):
        spread[side * QUARTER : (side + 1) * QUARTER, :] = jnp.dot(
            table[...], anom, preferred_element_type=F32
        )


def consume(chunk, bases, spread, index, weight, pair, first):
    for half in range(QUARTER // LANES):
        at = pl.multiple_of(chunk * QUARTER + half * LANES, LANES)
        lanes = slice(half * LANES, (half + 1) * LANES)
        acc = jnp.zeros((ROWS, LANES), F32)
        for n in range(0, index.shape[0], ROWS):
            idx = index[n : n + ROWS, pl.ds(at, LANES)]
            row = idx & (ROWS - 1)
            bits = [(idx & (ROWS << k)) != 0 for k in range(5)]
            block = idx >> 8
            value = jnp.zeros((ROWS, LANES), F32)
            for side, base in enumerate(bases):

                def got(v):
                    at_row = side * QUARTER + v * ROWS
                    return jnp.take_along_axis(
                        spread[at_row : at_row + ROWS, lanes], row, axis=0, mode="promise_in_bounds"
                    )

                value = jnp.where(block == base, choose(got, bits, 0, len(bits)), value)
            acc += value * weight[n : n + ROWS, pl.ds(at, LANES)]
        total = jnp.sum(acc, axis=0, keepdims=True)
        tile = chunk * (QUARTER // LANES) + half
        line = (tile >> 2) * ROWS + (tile & 3)
        pair[pl.ds(line, 1), :] = total if first is None else first[pl.ds(line, 1), :] + total


def pick(bases, tables, parts, index, weight, pair, first, even, odd):
    chunks = index.shape[1] // QUARTER
    slots = [even, odd]
    fill(0, tables, parts, even)
    for chunk in range(chunks):
        if chunk + 1 < chunks:
            fill(chunk + 1, tables, parts, slots[(chunk + 1) % 2])
        consume(chunk, bases, slots[chunk % 2], index, weight, pair, first)


def mid_kernel(lev, core, mid, *refs):
    parts, (index, weight, out, even, odd) = refs[:GROUPS], refs[GROUPS:]
    pick((GROUPS + lev[0],), (mid,), parts, index, weight, out, None, even, odd)


def mate_kernel(lev, core, mate, *refs):
    parts, (index, weight, first, out, even, odd) = refs[:GROUPS], refs[GROUPS:]
    side = jnp.where(core[0] == 0, 2, 0)
    pick((side * GROUPS + lev[0],), (mate,), parts, index, weight, out, first, even, odd)


def far_kernel(lev, core, far, *refs):
    anoms, parts = refs[:GROUPS], refs[GROUPS : 2 * GROUPS]
    index, weight, first = refs[2 * GROUPS : 2 * GROUPS + 3]
    outs, (spread, even, odd, pair) = refs[-GROUPS - 4 : -4], refs[-4:]
    group = lev[0]
    side = jnp.where(core[0] == 0, 0, 2)
    pick((side * GROUPS + group,), (far,), anoms, index, weight, pair, first, even, odd)
    kinds = lax.broadcasted_iota(jnp.int32, (NTYPE, LANES), 0).astype(F32)
    sums = jnp.zeros((NTYPE, LANES), F32)
    per = ROWS // 2
    for d, part in enumerate(parts):
        meta = part[2 * MEMBERS :, 0:LANES].astype(F32)
        share = pair[pl.ds(pl.multiple_of((group ^ d) * ROWS, ROWS), ROWS), :][0:per]
        share = share * (meta[0:per] + meta[per : 2 * per])
        for r in range(per):
            same = meta[2 * per + r : 2 * per + r + 1] == kinds
            sums += jnp.where(same, share[r : r + 1], 0.0)
    sums = jnp.sum(sums.T, axis=0, keepdims=True)
    tail = jnp.concatenate([sums, jnp.zeros((1, LANES - NTYPE), F32)], axis=1)
    spread[...] = jnp.broadcast_to(tail[None], spread.shape)
    for d, out in enumerate(outs):
        out[...] = pair[pl.ds(pl.multiple_of((group ^ d) * ROWS, ROWS), ROWS), :]


def finish_kernel(innovation, live, *refs):
    shares, impact = refs[:-1], refs[-1]
    lines = innovation.shape[0]
    pair = shares[0][0:lines, :]
    for share in shares[1:]:
        pair += share[0:lines, :]
    impact[...] = pair * innovation[...] * live[...].astype(F32) / (MEMBERS - 1.0)


def last_kernel(sums, impact, impact_out, type_out):
    total = jnp.sum(sums[...], axis=0)
    type_out[...] = total[:, 0:NTYPE]
    impact_out[...] = impact[...]


def steps(state_anom, error_sum, obs_anom, local_weight, neighbours, innovation, obs_type, live):
    lines = innovation.shape[0] // LANES
    lev = lax.axis_index("lev").reshape(1)
    core = lax.axis_index("col_2").reshape(1)

    def to_groups(blocks):
        got = [
            lax.ppermute(block, "lev", [(i, i ^ d) for i in range(GROUPS)])
            for d, block in enumerate(blocks)
            if d > 0
        ]
        return [near(block) for block in [blocks[0]] + got]

    send = pack(
        lev,
        state_anom,
        error_sum,
        innovation.reshape(lines, LANES),
        live.reshape(lines, LANES),
        obs_type.reshape(lines, LANES),
    )
    parts = to_groups(send)
    anoms = to_groups([obs_anom] * GROUPS)
    mid = total_sens(lev, parts)
    pairs = lax.axis_size(COL) // CORES
    odd_even = [(CORES * i + 1, CORES * i + 2) for i in range(pairs - 1)]
    far = lax.ppermute(mid, COL, odd_even + [(b, a) for a, b in odd_even])
    mate = lax.ppermute(mid, "col_2", [(0, 1), (1, 0)])
    index, weight = near(neighbours), near(local_weight)
    lists = GROUPS * ROWS
    cost = functools.partial(pl.CostEstimate, bytes_accessed=1 << 20, transcendentals=0)
    rows = dict(
        out_specs=VMEM,
        out_shape=pltpu.VMEM((lists, LANES), F32),
        scratch_shapes=[pltpu.VMEM((QUARTER, QUARTER), F32)] * 2,
        cost_estimate=cost(flops=1 << 26),
    )
    own = pl.pallas_call(
        mid_kernel, in_specs=[SMEM, SMEM] + [VMEM] * (GROUPS + 3), name="mid", **rows
    )(lev, core, near(mid), *anoms, index, weight)
    first = pl.pallas_call(
        mate_kernel, in_specs=[SMEM, SMEM] + [VMEM] * (GROUPS + 4), name="mate", **rows
    )(lev, core, near(mate), *anoms, index, weight, near(own))
    everyone = lax.axis_size(COL_LEV)
    *shares, spread = pl.pallas_call(
        far_kernel,
        in_specs=[SMEM, SMEM] + [VMEM] * (2 * GROUPS + 4),
        out_specs=[VMEM] * (GROUPS + 1),
        out_shape=[pltpu.VMEM((ROWS, LANES), F32)] * GROUPS
        + [jax.ShapeDtypeStruct((everyone, 1, LANES), F32)],
        scratch_shapes=[pltpu.VMEM((QUARTER, QUARTER), F32)] * 2 + [pltpu.VMEM((lists, LANES), F32)],
        cost_estimate=cost(flops=1 << 26),
        name="far",
    )(lev, core, near(far), *anoms, *parts, index, weight, near(first))
    sums = lax.all_to_all(spread, COL_LEV, 0, 0, tiled=True)
    impact = pl.pallas_call(
        finish_kernel,
        in_specs=[VMEM] * (GROUPS + 2),
        out_specs=VMEM,
        out_shape=pltpu.VMEM((lines, LANES), F32),
        name="finish",
    )(
        near(innovation.reshape(lines, LANES)),
        near(live.reshape(lines, LANES)),
        *to_groups(shares),
    )
    impact, type_impact = pl.pallas_call(
        last_kernel,
        in_specs=[VMEM] * 2,
        out_specs=[VMEM] * 2,
        out_shape=[
            jax.ShapeDtypeStruct((lines, LANES), F32),
            jax.ShapeDtypeStruct((1, NTYPE), F32),
        ],
        name="last",
    )(near(sums), near(impact))
    return (impact.reshape(-1), type_impact.reshape(-1))


def solution(mesh):
    split = Mesh(
        mesh.devices.reshape(4, 8, 2, mesh.shape["lev"]), ("col_0", "col_1", "col_2", "lev")
    )
    return jax.shard_map(
        steps,
        mesh=split,
        in_specs=(
            P("lev", None, COL),
            P("lev", COL),
            P("lev", COL),
            P(None, COL),
            P(None, COL),
            P(COL_LEV),
            P(COL_LEV),
            P(COL_LEV),
        ),
        out_specs=(P(COL_LEV), P()),
        check_vma=False,
    )
```

```python
import functools

import jax
import jax.numpy as jnp
from jax import lax
from jax.experimental import pallas as pl
from jax.experimental.pallas import tpu as pltpu
from jax.sharding import Mesh
from jax.sharding import PartitionSpec as P

MEMBERS = 64
NTYPE = 32
COL = ("col_0", "col_1", "col_2")
COL_LEV = ("col_0", "col_1", "col_2", "lev")
GROUPS = 4
CORES = 2
LANES = 128
ROWS = 8
QUARTER = 256
F32 = jnp.float32
BF16 = jnp.bfloat16
VMEM = pl.BlockSpec(memory_space=pltpu.VMEM)
SMEM = pl.BlockSpec(memory_space=pltpu.SMEM)
ANY = pl.BlockSpec(memory_space=pl.ANY)
FEWER_SPILLS = pltpu.CompilerParams(
)


def near(x):
    return pltpu.with_memory_space_constraint(x, pltpu.VMEM)


def halves(x, axis):
    hi = x.astype(BF16)
    lo = (x - hi.astype(F32)).astype(BF16)
    return jnp.concatenate([hi, lo], axis=axis)


def pack_kernel(lev, state, error, innovation, live, kind, *refs):
    outs, (s_buf, e_buf, m_buf, n_buf, sems) = refs[:GROUPS], refs[GROUPS:]
    levels = state.shape[0]
    order = (1, 2, 3, 0)
    starts = [pl.multiple_of((lev[0] ^ d) * QUARTER, QUARTER) for d in range(GROUPS)]
    small = [
        pltpu.make_async_copy(error, e_buf, sems.at[0]),
        pltpu.make_async_copy(innovation, m_buf.at[0], sems.at[1]),
        pltpu.make_async_copy(live, n_buf.at[0], sems.at[2]),
        pltpu.make_async_copy(kind, n_buf.at[1], sems.at[3]),
    ]
    parts = [
        pltpu.make_async_copy(state.at[:, :, pl.ds(starts[d], QUARTER)], s_buf.at[d], sems.at[4 + d])
        for d in range(GROUPS)
    ]
    small[0].start()
    parts[order[0]].start()
    for copy in small[1:]:
        copy.start()
    for d in order[1:]:
        parts[d].start()
    for copy in small:
        copy.wait()
    factor = m_buf[0] * n_buf[0].astype(F32) / (MEMBERS - 1.0)
    upper = factor.astype(BF16).astype(F32)
    meta = jnp.concatenate(
        [upper, factor - upper, n_buf[1].astype(F32), jnp.zeros_like(factor)], axis=0
    ).astype(BF16)
    meta = jnp.concatenate([meta, jnp.zeros_like(meta)], axis=1)
    for d in order:
        parts[d].wait()
        scale = e_buf[:, pl.ds(starts[d], QUARTER)]
        total = s_buf[d, 0].astype(F32) * scale[0:1]
        for level in range(1, levels):
            total += s_buf[d, level].astype(F32) * scale[level : level + 1]
        outs[d][0 : 2 * MEMBERS, :] = halves(total, 0)
        outs[d][2 * MEMBERS :, :] = meta


def pack(lev, state, error, innovation, live, kind):
    levels = state.shape[0]
    return pl.pallas_call(
        pack_kernel,
        in_specs=[SMEM] + [ANY] * 5,
        out_specs=[VMEM] * GROUPS,
        out_shape=[pltpu.VMEM((2 * MEMBERS + 16, QUARTER), BF16)] * GROUPS,
        scratch_shapes=[
            pltpu.VMEM((GROUPS, levels, MEMBERS, QUARTER), BF16),
            pltpu.VMEM(error.shape, F32),
            pltpu.VMEM((1,) + innovation.shape, F32),
            pltpu.VMEM((2,) + live.shape, jnp.int32),
            pltpu.SemaphoreType.DMA((4 + GROUPS,)),
        ],
        name="pack",
    )(lev, state, error, innovation, live, kind)


def total_kernel(lev, *refs):
    parts, out, held = refs[:GROUPS], refs[GROUPS], refs[GROUPS + 1]
    half = MEMBERS
    total = parts[0][0:half, :].astype(F32) + parts[0][half : 2 * half, :].astype(F32)
    for part in parts[1:]:
        total += part[0:half, :].astype(F32) + part[half : 2 * half, :].astype(F32)
    held[...] = total
    rows = MEMBERS // GROUPS
    total = jnp.concatenate(
        [held[pl.ds(pl.multiple_of((lev[0] ^ d) * rows, rows), rows), :] for d in range(GROUPS)],
        axis=0,
    )
    out[...] = halves(total.T, 1)


def total_sens(lev, parts):
    return pl.pallas_call(
        total_kernel,
        in_specs=[SMEM] + [VMEM] * GROUPS,
        out_specs=VMEM,
        out_shape=pltpu.VMEM((QUARTER, 2 * MEMBERS), BF16),
        scratch_shapes=[pltpu.VMEM((MEMBERS, QUARTER), F32)],
        name="total",
    )(lev, *parts)


def choose(got, bits, low, depth):
    if depth == 0:
        return got(low)
    upper = choose(got, bits, low + (1 << (depth - 1)), depth - 1)
    return jnp.where(bits[depth - 1], upper, choose(got, bits, low, depth - 1))


def fill(chunk, tables, parts, spread):
    at = pl.multiple_of(chunk * QUARTER, QUARTER)
    anom = jnp.concatenate([part[:, pl.ds(at, QUARTER)] for part in parts], axis=0)
    anom = jnp.concatenate([anom, anom], axis=0)
    for side, table in enumerate(tables):
        spread[side * QUARTER : (side + 1) * QUARTER, :] = jnp.dot(
            table[...], anom, preferred_element_type=F32
        )


def consume(chunk, bases, spread, index, weight, pair, first):
    for half in range(QUARTER // LANES):
        at = pl.multiple_of(chunk * QUARTER + half * LANES, LANES)
        lanes = slice(half * LANES, (half + 1) * LANES)
        acc = jnp.zeros((ROWS, LANES), F32)
        for n in range(0, index.shape[0], ROWS):
            idx = index[n : n + ROWS, pl.ds(at, LANES)]
            row = idx & (ROWS - 1)
            bits = [(idx & (ROWS << k)) != 0 for k in range(5)]
            block = idx >> 8
            value = jnp.zeros((ROWS, LANES), F32)
            for side, base in enumerate(bases):

                def got(v):
                    at_row = side * QUARTER + v * ROWS
                    return jnp.take_along_axis(
                        spread[at_row : at_row + ROWS, lanes], row, axis=0, mode="promise_in_bounds"
                    )

                value = jnp.where(block == base, choose(got, bits, 0, len(bits)), value)
            acc += value * weight[n : n + ROWS, pl.ds(at, LANES)]
        total = jnp.sum(acc, axis=0, keepdims=True)
        tile = chunk * (QUARTER // LANES) + half
        line = (tile >> 2) * ROWS + (tile & 3)
        pair[pl.ds(line, 1), :] = total if first is None else first[pl.ds(line, 1), :] + total


def pick(bases, tables, parts, index, weight, pair, first, even, odd):
    chunks = index.shape[1] // QUARTER
    slots = [even, odd]
    fill(0, tables, parts, even)
    for chunk in range(chunks):
        if chunk + 1 < chunks:
            fill(chunk + 1, tables, parts, slots[(chunk + 1) % 2])
        consume(chunk, bases, slots[chunk % 2], index, weight, pair, first)


def mid_kernel(lev, core, mid, *refs):
    parts, (index, weight, out, even, odd) = refs[:GROUPS], refs[GROUPS:]
    pick((GROUPS + lev[0],), (mid,), parts, index, weight, out, None, even, odd)


def mate_kernel(lev, core, mate, *refs):
    parts, (index, weight, first, out, even, odd) = refs[:GROUPS], refs[GROUPS:]
    side = jnp.where(core[0] == 0, 2, 0)
    pick((side * GROUPS + lev[0],), (mate,), parts, index, weight, out, first, even, odd)


def far_kernel(lev, core, far, *refs):
    anoms, parts = refs[:GROUPS], refs[GROUPS : 2 * GROUPS]
    index, weight, first = refs[2 * GROUPS : 2 * GROUPS + 3]
    outs, (spread, even, odd, pair) = refs[-GROUPS - 4 : -4], refs[-4:]
    group = lev[0]
    side = jnp.where(core[0] == 0, 0, 2)
    pick((side * GROUPS + group,), (far,), anoms, index, weight, pair, first, even, odd)
    kinds = lax.broadcasted_iota(jnp.int32, (NTYPE, LANES), 0).astype(F32)
    sums = jnp.zeros((NTYPE, LANES), F32)
    per = ROWS // 2
    for d, part in enumerate(parts):
        meta = part[2 * MEMBERS :, 0:LANES].astype(F32)
        share = pair[pl.ds(pl.multiple_of((group ^ d) * ROWS, ROWS), ROWS), :][0:per]
        share = share * (meta[0:per] + meta[per : 2 * per])
        for r in range(per):
            same = meta[2 * per + r : 2 * per + r + 1] == kinds
            sums += jnp.where(same, share[r : r + 1], 0.0)
    sums = jnp.sum(sums.T, axis=0, keepdims=True)
    tail = jnp.concatenate([sums, jnp.zeros((1, LANES - NTYPE), F32)], axis=1)
    spread[...] = jnp.broadcast_to(tail[None], spread.shape)
    for d, out in enumerate(outs):
        out[...] = pair[pl.ds(pl.multiple_of((group ^ d) * ROWS, ROWS), ROWS), :]


def finish_kernel(innovation, live, *refs):
    shares, impact = refs[:-1], refs[-1]
    lines = innovation.shape[0]
    pair = shares[0][0:lines, :]
    for share in shares[1:]:
        pair += share[0:lines, :]
    impact[...] = pair * innovation[...] * live[...].astype(F32) / (MEMBERS - 1.0)


def last_kernel(sums, impact, impact_out, type_out):
    total = jnp.sum(jnp.sum(sums[...], axis=0), axis=0, keepdims=True)
    type_out[...] = total[:, 0:NTYPE]
    impact_out[...] = impact[...]


def steps(state_anom, error_sum, obs_anom, local_weight, neighbours, innovation, obs_type, live):
    lines = innovation.shape[0] // LANES
    lev = lax.axis_index("lev").reshape(1)
    core = lax.axis_index("col_2").reshape(1)

    def to_groups(blocks):
        got = [blocks[0]]
        for d in range(1, GROUPS):
            got.append(lax.ppermute(blocks[d], "lev", [(i, i ^ d) for i in range(GROUPS)]))
        return [near(block) for block in got]

    send = pack(
        lev,
        state_anom,
        error_sum,
        innovation.reshape(lines, LANES),
        live.reshape(lines, LANES),
        obs_type.reshape(lines, LANES),
    )
    parts = to_groups(send)
    anoms = to_groups([obs_anom] * GROUPS)
    mid = total_sens(lev, parts)
    pairs = lax.axis_size(COL) // CORES
    odd_even = [(CORES * i + 1, CORES * i + 2) for i in range(pairs - 1)]
    far = lax.ppermute(mid, COL, odd_even + [(b, a) for a, b in odd_even])
    mate = lax.ppermute(mid, "col_2", [(0, 1), (1, 0)])
    index, weight = near(neighbours), near(local_weight)
    lists = GROUPS * ROWS
    cost = functools.partial(pl.CostEstimate, bytes_accessed=1 << 20, transcendentals=0)
    rows = dict(
        out_specs=VMEM,
        out_shape=pltpu.VMEM((lists, LANES), F32),
        scratch_shapes=[pltpu.VMEM((QUARTER, QUARTER), F32)] * 2,
        cost_estimate=cost(flops=1 << 26),
        compiler_params=FEWER_SPILLS,
    )
    own = pl.pallas_call(
        mid_kernel, in_specs=[SMEM, SMEM] + [VMEM] * (GROUPS + 3), name="mid", **rows
    )(lev, core, near(mid), *anoms, index, weight)
    first = pl.pallas_call(
        mate_kernel, in_specs=[SMEM, SMEM] + [VMEM] * (GROUPS + 4), name="mate", **rows
    )(lev, core, near(mate), *anoms, index, weight, near(own))
    everyone = lax.axis_size(COL_LEV)
    *shares, spread = pl.pallas_call(
        far_kernel,
        in_specs=[SMEM, SMEM] + [VMEM] * (2 * GROUPS + 4),
        out_specs=[VMEM] * (GROUPS + 1),
        out_shape=[pltpu.VMEM((ROWS, LANES), F32)] * GROUPS
        + [jax.ShapeDtypeStruct((everyone // ROWS, ROWS, LANES), F32)],
        scratch_shapes=[pltpu.VMEM((QUARTER, QUARTER), F32)] * 2 + [pltpu.VMEM((lists, LANES), F32)],
        cost_estimate=cost(flops=1 << 26),
        compiler_params=FEWER_SPILLS,
        name="far",
    )(lev, core, near(far), *anoms, *parts, index, weight, near(first))
    sums = lax.all_to_all(spread.reshape(everyone, 1, LANES), COL_LEV, 0, 0, tiled=True)
    sums = sums.reshape(everyone // ROWS, ROWS, LANES)
    impact = pl.pallas_call(
        finish_kernel,
        in_specs=[VMEM] * (GROUPS + 2),
        out_specs=VMEM,
        out_shape=pltpu.VMEM((lines, LANES), F32),
        name="finish",
    )(
        near(innovation.reshape(lines, LANES)),
        near(live.reshape(lines, LANES)),
        *to_groups(shares),
    )
    impact, type_impact = pl.pallas_call(
        last_kernel,
        in_specs=[VMEM] * 2,
        out_specs=[VMEM] * 2,
        out_shape=[
            jax.ShapeDtypeStruct((lines, LANES), F32),
            jax.ShapeDtypeStruct((1, NTYPE), F32),
        ],
        name="last",
    )(near(sums), near(impact))
    return (impact.reshape(-1), type_impact.reshape(-1))


def solution(mesh):
    split = Mesh(
        mesh.devices.reshape(4, 8, 2, mesh.shape["lev"]), ("col_0", "col_1", "col_2", "lev")
    )
    return jax.shard_map(
        steps,
        mesh=split,
        in_specs=(
            P("lev", None, COL),
            P("lev", COL),
            P("lev", COL),
            P(None, COL),
            P(None, COL),
            P(COL_LEV),
            P(COL_LEV),
            P(COL_LEV),
        ),
        out_specs=(P(COL_LEV), P()),
        check_vma=False,
    )
```
